32 devices in a mesh: az: 8 (over z, y), rg: 4 (over x, core).
Axes of the slice: x: 2, y: 2, z: 4, core: 2. Of those that a mesh axis runs over, the one named last changes fastest.
Arguments:
- ref_image: float32 [1024, 3072], P('az', 'rg'), may hold values from 0.2 to 5
- sec_image: float32 [1024, 3072], P('az', 'rg'), may hold values from 0.2 to 5
- off_az: int32 [16], P('az'), may hold values from -7 to 7, as said below
- off_rg: int32 [16], P('az'), may hold values from -7 to 7, as said below
Outputs:
- surfaces: float32 [16, 48, 128, 128], P('az', 'rg')
The draws below stay inside these ranges and needn't reach their ends.
Inputs may be any that keep to these rules, and one draw needn't show every extreme that they name: off_az is monotone over the chip rows, changes by 0 or 1 between neighbouring chip rows, and runs from one end of its range to the other. off_rg is monotone over the chip rows, changes by 0 or 1 between neighbouring chip rows, and runs from one end of its range to the other.
All inputs are finite; a program needn't handle non-finite values.
Results may differ from the reference program's by a relative error of at most 0.0003.
Values sent between devices are 32-bit elements; how exact they have to be, the bound alone decides.
No kernel may reach another device: no remote copies, remote signals or barrier semaphores. Data moves between devices by JAX's collectives and lax.ppermute only.
A program may use at most 64 MiB of HBM per device.

```python
import math
import jax
import jax.numpy as jnp
from jax import lax

CHIP = 128
SPACE = 64
SEARCH = 192
LAGS = 64
A_DEV = 128
NA = 1024
NR = 3072
NKA = 16
OFFAZ = 7
OFFRG = 7


def monotone_path(key, count, reach):
    order = jax.random.permutation(key, count - 1)
    steps = (order < 2 * reach).astype(jnp.int32)
    path = jnp.concatenate([jnp.zeros((1,), jnp.int32), jnp.cumsum(steps).astype(jnp.int32)]) - reach
    flip = jax.random.randint(jax.random.fold_in(key, 5), (), 0, 2, dtype=jnp.int32)
    return jnp.where(flip == 1, -path, path).astype(jnp.int32)


def draw_off_az(key, part):
    return monotone_path(jax.random.fold_in(key, 11), NKA, OFFAZ)


def draw_off_rg(key, part):
    return monotone_path(jax.random.fold_in(key, 23), NKA, OFFRG)


def block_levels(rng, dims, split, least, largest):
    loudness = 1.0
    for position, shards_of in split:
        steps = jax.random.uniform(jax.random.fold_in(jax.random.fold_in(rng, 6), position), (shards_of,), jnp.float32, least / len(split), largest / len(split))
        loudness = loudness * jnp.repeat(jnp.exp(steps), dims[position] // shards_of).reshape((-1,) + (1,) * (len(dims) - 1 - position))
    return loudness


def setup_inputs(seed: int = 0) -> dict:
    keys = jax.random.split(jax.random.key(seed), 5)
    ref_image = jnp.clip(jnp.exp(math.log(5.0) - 3.218876 * jax.random.uniform(keys[0], (NA, NR), jnp.float32) ** block_levels(keys[0], (NA, NR), ((0, 8), (1, 4)), -0.2, 0.2)), 0.2, 5.0)
    sec_image = jnp.clip(jnp.exp(math.log(5.0) - 3.218876 * jax.random.uniform(keys[1], (NA, NR), jnp.float32) ** block_levels(keys[1], (NA, NR), ((0, 8), (1, 4)), -0.2, 0.2)), 0.2, 5.0)
    off_az = draw_off_az(jax.random.fold_in(keys[4], 71), 0)
    off_rg = draw_off_rg(jax.random.fold_in(keys[4], 71), 0)
    return {"ref_image": ref_image, "sec_image": sec_image, "off_az": off_az, "off_rg": off_rg}


EPSILON = 1e-06
HIGH = lax.Precision.HIGHEST

def box_matrix():
    lag_index = lax.iota(jnp.int32, LAGS)[:, None]
    cell_index = lax.iota(jnp.int32, SEARCH)[None, :]
    return ((cell_index >= lag_index) & (cell_index < lag_index + CHIP)).astype(jnp.float32)

def cubic_matrix():
    out_index = lax.iota(jnp.int32, 2 * LAGS)[:, None]
    sample = lax.iota(jnp.int32, LAGS)[None, :]
    base = out_index // 2

    def pick(where):
        return (jnp.clip(where, 0, LAGS - 1) == sample).astype(jnp.float32)
    even_part = pick(base)
    odd_part = (9.0 * (pick(base) + pick(base + 1)) - (pick(base - 1) + pick(base + 2))) / 16.0
    return jnp.where(out_index % 2 == 1, odd_part, even_part)

def cut_chips(band, count):
    blocks = band.reshape(band.shape[0], count + 1, SPACE)
    joined = jnp.concatenate([blocks[:, :-1], blocks[:, 1:]], axis=2)
    return jnp.transpose(joined, (1, 0, 2))

def cut_windows(band, count):
    blocks = band.reshape(band.shape[0], count + 2, SPACE)
    joined = jnp.concatenate([blocks[:, :-2], blocks[:, 1:-1], blocks[:, 2:]], axis=2)
    return jnp.transpose(joined, (1, 0, 2))

def finish(corr, centered, windows):
    box_sum = box_matrix()
    first = jnp.einsum('pr,nrs->nps', box_sum, windows, precision=HIGH)
    first = jnp.einsum('nps,qs->npq', first, box_sum, precision=HIGH)
    second = jnp.einsum('pr,nrs->nps', box_sum, windows * windows, precision=HIGH)
    second = jnp.einsum('nps,qs->npq', second, box_sum, precision=HIGH)
    area = float(CHIP * CHIP)
    var_sum = second - first * first / area
    energy = lax.optimization_barrier(jnp.sum(centered * centered, axis=(1, 2)))
    score = CHIP * (corr / area) / jnp.sqrt(energy[:, None, None] / area * (var_sum / area) + EPSILON)
    oversample = cubic_matrix()
    lifted = jnp.einsum('ap,npq->naq', oversample, score, precision=HIGH)
    return jnp.einsum('naq,bq->nab', lifted, oversample, precision=HIGH)

def reference(ref_image, sec_image, off_az, off_rg):
    quarter = CHIP // 4
    half_chip = CHIP // 2
    ref_pad = jnp.pad(ref_image, quarter)
    sec_pad = jnp.pad(sec_image, ((A_DEV, A_DEV), (CHIP, CHIP)))
    total_rows = ref_image.shape[0] // SPACE
    chip_cols = ref_image.shape[1] // SPACE

    def one_row(inputs):
        row_index, shift_az, shift_rg = inputs
        ref_band = lax.dynamic_slice_in_dim(ref_pad, row_index * SPACE, CHIP, 0)
        chips = cut_chips(ref_band, chip_cols)
        sec_rows = lax.dynamic_slice_in_dim(sec_pad, row_index * SPACE + shift_az - half_chip + A_DEV, SEARCH, 0)
        sec_band = lax.dynamic_slice_in_dim(sec_rows, shift_rg + half_chip, chip_cols * SPACE + CHIP, 1)
        windows = cut_windows(sec_band, chip_cols)
        centered = chips - lax.optimization_barrier(jnp.mean(chips, axis=(1, 2), keepdims=True))
        padded = jnp.pad(centered, ((0, 0), (0, SEARCH - CHIP), (0, SEARCH - CHIP)))
        spectrum = jnp.conj(jnp.fft.fft2(padded)) * jnp.fft.fft2(windows)
        corr = jnp.real(jnp.fft.ifft2(spectrum))[:, :LAGS, :LAGS]
        return finish(corr, centered, windows)
    row_list = lax.iota(jnp.int32, total_rows)
    return lax.map(one_row, (row_list, off_az, off_rg))
```

```python
import functools
import math

import jax
import jax.numpy as jnp
import numpy as np
from jax import lax
from jax.experimental import pallas as pl
from jax.experimental.pallas import tpu as pltpu
from jax.sharding import PartitionSpec as P

CHIP = 128
SPACE = 64
SEARCH = 192
LAGS = 64
LANES = 128
FREQ = SEARCH // 2
EPSILON = 1e-06
AREA = float(CHIP * CHIP)
BF16 = jnp.bfloat16
F32 = jnp.float32


def halves(table):
    high = table.astype(BF16)
    low = (table - high.astype(np.float64)).astype(BF16)
    return high, low


@functools.cache
def tables():
    theta = 2.0 * math.pi * (np.arange(FREQ)[:, None] + 0.5) / SEARCH
    cell = np.arange(SEARCH)[None, :]
    forward = np.concatenate([np.cos(theta * cell), -np.sin(theta * cell)], axis=0)
    lag = np.arange(LAGS)[:, None]
    box = ((cell >= lag) & (cell < lag + CHIP)).astype(np.float64)
    high, low = halves(np.concatenate([forward, box], axis=0))
    rows_sec = np.concatenate([high, high, low], axis=1)
    high, low = halves(forward[:, :CHIP])
    rows_ref = np.concatenate([high, high, low], axis=1)
    rows_box = np.concatenate([box, box], axis=1).astype(BF16)

    phi = 2.0 * math.pi / CHIP * np.arange(CHIP)[None, :]
    spot = np.arange(SPACE)[:, None]
    cosine, sine = np.cos(phi * spot), np.sin(phi * spot)
    block = np.concatenate(
        [np.concatenate([cosine, -sine], axis=1), np.concatenate([sine, cosine], axis=1)], axis=0
    )
    spread = np.zeros((4 * SPACE, 4 * CHIP))
    for half in range(2):
        for part in range(2):
            spread[2 * SPACE * part + SPACE * half:][:SPACE, 2 * CHIP * half:][:, : 2 * CHIP] = block[
                SPACE * part:][:SPACE]
    high, low = halves(spread)
    columns = np.concatenate([high, high, low], axis=0)

    back = np.zeros((4 * CHIP, 4 * LAGS))
    cosine, sine = np.cos(phi.T * lag.T), np.sin(phi.T * lag.T)
    for half in range(2):
        base = 2 * CHIP * half
        back[base:base + CHIP, LAGS * half:LAGS * (half + 1)] = cosine
        back[base:base + CHIP, LAGS * (2 + half):LAGS * (3 + half)] = sine
        back[base + CHIP:base + 2 * CHIP, LAGS * half:LAGS * (half + 1)] = -sine
        back[base + CHIP:base + 2 * CHIP, LAGS * (2 + half):LAGS * (3 + half)] = cosine
    high, low = halves(back)
    back_columns = np.concatenate([high, high, low], axis=0)

    final = np.concatenate([np.cos(theta.T * lag), -np.sin(theta.T * lag)], axis=1)
    high, low = halves(final * (2.0 / (SEARCH * CHIP)))
    back_rows = np.concatenate([high, high, low], axis=1)

    wide = np.arange(2 * LANES)[:, None]
    lane = np.arange(LANES)[None, :]
    slide = ((wide >= lane) & (wide < lane + CHIP)).astype(np.float64)
    start = lane // SPACE * SPACE
    gather = ((wide >= start) & (wide < start + CHIP)).astype(np.float64)
    slide = np.concatenate([slide, slide], axis=0).astype(BF16)
    gather = np.concatenate([gather, gather, gather], axis=0).astype(BF16)

    out_index = np.arange(2 * LAGS)[:, None]
    sample = np.arange(LAGS)[None, :]
    base = out_index // 2

    def pick(where):
        return (np.clip(where, 0, LAGS - 1) == sample).astype(np.float64)

    odd = (9.0 * (pick(base) + pick(base + 1)) - (pick(base - 1) + pick(base + 2))) / 16.0
    cubic = np.where(out_index % 2 == 1, odd, pick(base))
    cubic_rows = np.concatenate([cubic, cubic], axis=1).astype(BF16)
    zero = np.zeros_like(cubic.T)
    pair = np.concatenate(
        [np.concatenate([cubic.T, zero], axis=1), np.concatenate([zero, cubic.T], axis=1)], axis=0
    )
    cubic_cols = np.concatenate([pair, pair], axis=0).astype(BF16)
    return (rows_sec, rows_ref, rows_box, columns, back_columns, back_rows, slide, gather,
            cubic_rows, cubic_cols)


def split(value):
    high = value.astype(BF16)
    low = (value - high.astype(F32)).astype(BF16)
    return high, low


def dot(left, right):
    return jnp.dot(left, right, preferred_element_type=F32)


def pack_kernel(pad, side, sec_l, sec_r, ref_l, ref_r, up_l, up_r, down_l, down_r, right_out, left_out):
    rows = sec_l.shape[0]
    lane = lax.broadcasted_iota(jnp.int32, (1, LANES), 1)

    def tile(out, up, sec, down, ref, shift, keep):
        out[0:pad] = up[0:pad]
        out[pad:pad + rows] = sec[...]
        out[pad + rows:pad + rows + pad] = down[0:pad]
        inner = jnp.concatenate([up[pad:pad + side], ref[...], down[pad:pad + side]], axis=0)
        here = slice(pad - side, pad + rows + side)
        out[here] = jnp.where(keep, out[here], pltpu.roll(inner, shift, 1))

    tile(right_out, up_r, sec_r, down_r, ref_r, side, lane >= side)
    tile(left_out, up_l, sec_l, down_l, ref_l, LANES - side, lane < LANES - side)


def main_kernel(pad, side, off_az, off_rg, sec, ref, up, down, left, right, rows_sec, rows_ref, rows_box,
                columns, back_columns, back_rows, slide, gather, cubic_rows, cubic_cols, out,
                sec_ext, ref_ext, lhs, spec, zed):
    rows, cols = sec.shape
    tiles = cols // LANES
    step = pl.program_id(0)
    width = cols + 2 * LANES
    band = cols + LANES

    @pl.when(step == 0)
    def _():
        level_sec = jnp.sum(sec[...]) * (1.0 / (rows * cols))
        level_ref = jnp.sum(ref[...]) * (1.0 / (rows * cols))
        inner = slice(LANES, LANES + cols)
        sec_ext[0:pad, inner] = up[0:pad] - level_sec
        sec_ext[pad:pad + rows, inner] = sec[...] - level_sec
        sec_ext[pad + rows:, inner] = down[0:pad] - level_sec
        sec_ext[:, 0:LANES] = left[...] - level_sec
        sec_ext[:, LANES + cols:] = right[...] - level_sec
        here = slice(pad - side, pad + rows + side)
        middle = jnp.concatenate([up[pad:pad + side], ref[...], down[pad:pad + side]], axis=0)
        whole = jnp.concatenate(
            [pltpu.roll(left[here], LANES - side, 1), middle, pltpu.roll(right[here], side, 1)], axis=1)
        ref_ext[...] = pltpu.roll(whole, width - (LANES - side), 1)[:, :band] - level_ref

    start = step * SPACE + (pad - SPACE) + off_az[step]
    aligned = pl.multiple_of(start // 8 * 8, 8)
    field = sec_ext[pl.ds(aligned, SEARCH + 8), :]
    field = pltpu.roll(field, width - SPACE - off_rg[step], 1)[:, :band]
    field = pltpu.roll(field, SEARCH + 8 - (start - aligned), 0)[:SEARCH]
    high, low = split(field)
    spectrum = dot(rows_sec[...], jnp.concatenate([high, low, high], axis=0))
    square_high, square_low = split(field * field)
    second = dot(rows_box[...], jnp.concatenate([square_high, square_low], axis=0))
    first = spectrum[2 * FREQ:]
    chips = ref_ext[pl.ds(pl.multiple_of(step * SPACE, SPACE), CHIP), :]
    high, low = split(chips)
    chip_spectrum = dot(rows_ref[...], jnp.concatenate([high, low, high], axis=0))
    count = tiles + 1
    for which, source in enumerate((spectrum, chip_spectrum)):
        for t in range(count):
            here = slice(t * LANES, (t + 1) * LANES)
            both = jnp.concatenate([source[:FREQ, here], source[FREQ:2 * FREQ, here]], axis=1)
            high, low = split(both)
            row = (which * count + t) * FREQ
            lhs[row:row + FREQ, :] = jnp.concatenate([high, low], axis=1)
    both = lhs[...]
    spec[...] = dot(jnp.concatenate([both, both[:, :2 * LANES]], axis=1), columns[...])

    sign = (1 - 2 * (lax.broadcasted_iota(jnp.int32, (1, LANES), 1) % 2)).astype(F32)

    def block(which, b):
        row = (which * count + b // 2) * FREQ
        base = 2 * CHIP * (b % 2)
        return spec[row:row + FREQ, base:base + CHIP], spec[row:row + FREQ, base + CHIP:base + 2 * CHIP]

    def product(b):
        (w_re, w_im), (n_re, n_im), (c_re, c_im) = block(0, b), block(0, b + 1), block(1, b)
        p_re, p_im = w_re + sign * n_re, w_im + sign * n_im
        return c_re * p_re + c_im * p_im, c_re * p_im - c_im * p_re

    chips_here = 2 * tiles
    before = product(0)
    for c in range(chips_here):
        after = product(c + 1)
        both = jnp.concatenate([before[0] + after[0], before[1] + after[1]], axis=1)
        high, low = split(both)
        row, base = (c // 2) * FREQ, 2 * CHIP * (c % 2)
        zed[row:row + FREQ, base:base + 2 * CHIP] = high
        zed[row:row + FREQ, 4 * CHIP + base:4 * CHIP + base + 2 * CHIP] = low
        before = after
    both = zed[...]
    lags = dot(jnp.concatenate([both, both[:, :4 * CHIP]], axis=1), back_columns[...])
    pieces = [lags[t * FREQ:(t + 1) * FREQ] for t in range(tiles)]
    stacked = jnp.concatenate(
        [jnp.concatenate([piece[:, :LANES], piece[:, LANES:]], axis=0) for piece in pieces], axis=1)
    high, low = split(stacked)
    raw = dot(back_rows[...], jnp.concatenate([high, low, high], axis=0))

    sums = jnp.concatenate([first, second], axis=0)
    sums = jnp.concatenate([sums[:, t * LANES:(t + 2) * LANES] for t in range(tiles)], axis=0)
    high, low = split(sums)
    boxes = dot(jnp.concatenate([high, low], axis=1), slide[...])
    totals = jnp.concatenate(
        [jnp.sum(chips.reshape(CHIP // 8, 8, band), axis=0),
         jnp.sum((chips * chips).reshape(CHIP // 8, 8, band), axis=0)], axis=0)
    totals = jnp.concatenate([totals[:, t * LANES:(t + 2) * LANES] for t in range(tiles)], axis=0)
    high, low = split(totals)
    rest = (totals - high.astype(F32) - low.astype(F32)).astype(BF16)
    totals = dot(jnp.concatenate([high, low, rest], axis=1), gather[...])

    scores = []
    for t in range(tiles):
        first_t = boxes[t * CHIP:t * CHIP + LAGS]
        second_t = boxes[t * CHIP + LAGS:(t + 1) * CHIP]
        total = jnp.sum(totals[16 * t:16 * t + 8], axis=0, keepdims=True)
        power = jnp.sum(totals[16 * t + 8:16 * t + 16], axis=0, keepdims=True)
        corr = raw[:, t * LANES:(t + 1) * LANES] - (total * (1.0 / AREA)) * first_t
        var_sum = second_t - first_t * first_t * (1.0 / AREA)
        energy = power - total * total * (1.0 / AREA)
        scores.append(CHIP * (corr * (1.0 / AREA)) * lax.rsqrt(
            (energy * (1.0 / AREA)) * (var_sum * (1.0 / AREA)) + EPSILON))
    high, low = split(jnp.concatenate(scores, axis=1))
    lifted = dot(cubic_rows[...], jnp.concatenate([high, low], axis=0))
    lifted = jnp.concatenate([lifted[:, t * LANES:(t + 1) * LANES] for t in range(tiles)], axis=0)
    high, low = split(lifted)
    fine = dot(jnp.concatenate([high, low], axis=1), cubic_cols[...])
    for c in range(chips_here):
        row, base = (c // 2) * CHIP, CHIP * (c % 2)
        out[0, c] = fine[row:row + CHIP, base:base + CHIP]


def neighbours(axis):
    size = lax.axis_size(axis)
    forth = [(i, i + 1) for i in range(size - 1)]
    return forth, [(j, i) for i, j in forth]


def body(ref_image, sec_image, off_az, off_rg):
    rows, cols = ref_image.shape
    side = CHIP // 4
    chip_rows, chip_cols = rows // SPACE, cols // SPACE
    all_rows = chip_rows * lax.axis_size("az")
    reach = min(SPACE - 1, (all_rows - 1) // 2)
    pad = -(-(SPACE + reach) // 8) * 8
    assert SPACE + reach + side <= LANES
    tiles = cols // LANES

    forth, back = neighbours("az")
    up = lax.ppermute(jnp.concatenate([sec_image[rows - pad:], ref_image[rows - side:]], axis=0), "az", forth)
    down = lax.ppermute(jnp.concatenate([sec_image[:pad], ref_image[:side]], axis=0), "az", back)

    tall = rows + 2 * pad

    def end(index, height):
        return pl.BlockSpec((height, LANES), lambda i, index=index: (0, index))

    ends = [end(i, h) for h in (rows, rows, pad + side, pad + side) for i in (0, tiles - 1)]
    to_right, to_left = pl.pallas_call(
        functools.partial(pack_kernel, pad, side),
        grid=(1,),
        in_specs=ends,
        out_specs=[pl.BlockSpec((tall, LANES), lambda i: (0, 0))] * 2,
        out_shape=[jax.ShapeDtypeStruct((tall, LANES), F32)] * 2,
    )(sec_image, sec_image, ref_image, ref_image, up, up, down, down)
    forth, back = neighbours("rg")
    left = lax.ppermute(to_right, "rg", forth)
    right = lax.ppermute(to_left, "rg", back)

    constants = [jnp.asarray(t) for t in tables()]
    operands = [sec_image, ref_image, up, down, left, right, *constants]
    count = tiles + 1

    def whole(x):
        return pl.BlockSpec(x.shape, lambda i, *_: (0, 0), pipeline_mode=pl.Buffered(1))

    return pl.pallas_call(
        functools.partial(main_kernel, pad, side),
        grid_spec=pltpu.PrefetchScalarGridSpec(
            num_scalar_prefetch=2,
            grid=(chip_rows,),
            in_specs=[whole(x) for x in operands],
            out_specs=pl.BlockSpec((1, chip_cols, 2 * LAGS, 2 * LAGS), lambda i, *_: (i, 0, 0, 0)),
            scratch_shapes=[
                pltpu.VMEM((tall, cols + 2 * LANES), F32),
                pltpu.VMEM((rows + 2 * side, cols + LANES), F32),
                pltpu.VMEM((2 * count * FREQ, 4 * LANES), BF16),
                pltpu.VMEM((2 * count * FREQ, 4 * CHIP), F32),
                pltpu.VMEM((tiles * FREQ, 8 * CHIP), BF16),
            ],
        ),
        out_shape=jax.ShapeDtypeStruct((chip_rows, chip_cols, 2 * LAGS, 2 * LAGS), F32),
        compiler_params=pltpu.CompilerParams(dimension_semantics=("arbitrary",), vmem_limit_bytes=48 << 20),
    )(off_az, off_rg, *operands)


def solution(mesh):
    return jax.shard_map(
        body,
        mesh=mesh,
        in_specs=(P("az", "rg"), P("az", "rg"), P("az"), P("az")),
        out_specs=P("az", "rg", None, None),
        check_vma=False,
    )
```

```python
import functools
import math

import jax
import jax.numpy as jnp
import numpy as np
from jax import lax
from jax.experimental import pallas as pl
from jax.experimental.pallas import tpu as pltpu
from jax.sharding import PartitionSpec as P

CHIP = 128
SPACE = 64
SEARCH = 192
LAGS = 64
LANES = 128
FREQ = SEARCH // 2
EPSILON = 1e-06
AREA = float(CHIP * CHIP)
BF16 = jnp.bfloat16
F32 = jnp.float32


def halves(table):
    high = table.astype(BF16)
    low = (table - high.astype(np.float64)).astype(BF16)
    return high, low


@functools.cache
def tables():
    theta = 2.0 * math.pi * (np.arange(FREQ)[:, None] + 0.5) / SEARCH
    cell = np.arange(SEARCH)[None, :]
    forward = np.concatenate([np.cos(theta * cell), -np.sin(theta * cell)], axis=0)
    lag = np.arange(LAGS)[:, None]
    box = ((cell >= lag) & (cell < lag + CHIP)).astype(np.float64)
    made = {}
    high, low = halves(np.concatenate([forward, box], axis=0))
    made["rows_sec"] = np.concatenate([high, high, low], axis=1)
    high, low = halves(forward[:, :CHIP])
    made["rows_ref"] = np.concatenate([high, high, low], axis=1)
    made["rows_box"] = np.concatenate([box, box], axis=1).astype(BF16)

    phi = 2.0 * math.pi / CHIP * np.arange(CHIP)[None, :]
    spot = np.arange(SPACE)[:, None]
    cosine, sine = np.cos(phi * spot), np.sin(phi * spot)
    parts = (np.concatenate([cosine, -sine], axis=1), np.concatenate([sine, cosine], axis=1))
    spread = np.zeros((4 * SPACE, 4 * CHIP))
    for half in range(2):
        for part in range(2):
            row = 2 * SPACE * part + SPACE * half
            spread[row:row + SPACE, 2 * CHIP * half:2 * CHIP * (half + 1)] = parts[part]
    made["columns"] = np.concatenate(halves(spread), axis=0)

    back = np.zeros((4 * CHIP, 4 * LAGS))
    cosine, sine = np.cos(phi.T * lag.T), np.sin(phi.T * lag.T)
    for half in range(2):
        base = 2 * CHIP * half
        back[base:base + CHIP, LAGS * half:LAGS * (half + 1)] = cosine
        back[base:base + CHIP, LAGS * (2 + half):LAGS * (3 + half)] = sine
        back[base + CHIP:base + 2 * CHIP, LAGS * half:LAGS * (half + 1)] = -sine
        back[base + CHIP:base + 2 * CHIP, LAGS * (2 + half):LAGS * (3 + half)] = cosine
    made["back_columns"] = np.concatenate(halves(back), axis=0)

    final = np.concatenate([np.cos(theta.T * lag), -np.sin(theta.T * lag)], axis=1)
    high, low = halves(final * (2.0 / (SEARCH * CHIP)))
    made["back_rows"] = np.concatenate([high, high, low], axis=1)

    wide = np.arange(2 * LANES)[:, None]
    lane = np.arange(LANES)[None, :]
    start = lane // SPACE * SPACE
    made["slide"] = ((wide >= lane) & (wide < lane + CHIP)).astype(BF16)
    made["gather"] = ((wide >= start) & (wide < start + CHIP)).astype(BF16)

    out_index = np.arange(2 * LAGS)[:, None]
    sample = np.arange(LAGS)[None, :]
    base = out_index // 2

    def pick(where):
        return (np.clip(where, 0, LAGS - 1) == sample).astype(np.float64)

    odd = (9.0 * (pick(base) + pick(base + 1)) - (pick(base - 1) + pick(base + 2))) / 16.0
    cubic = np.where(out_index % 2 == 1, odd, pick(base))
    made["cubic_rows"] = np.concatenate([cubic, cubic], axis=1).astype(BF16)
    zero = np.zeros_like(cubic.T)
    made["cubic_cols"] = np.concatenate(
        [np.concatenate([cubic.T, zero], axis=1), np.concatenate([zero, cubic.T], axis=1)], axis=0
    ).astype(BF16)

    slabs, places, top = [], {}, 0
    for name, table in made.items():
        table = np.pad(table, ((0, 0), (0, -table.shape[1] % LANES)))
        pieces = [table[:, i:i + LANES] for i in range(0, table.shape[1], LANES)]
        places[name] = (top, table.shape[0], len(pieces), made[name].shape[1])
        slabs += pieces
        top += table.shape[0] * len(pieces)
    return np.concatenate(slabs, axis=0), places


def split(value):
    high = value.astype(BF16)
    low = (value - high.astype(F32)).astype(BF16)
    return high, low


def dot(left, right):
    return jnp.dot(left, right, preferred_element_type=F32)


def pack_kernel(pad, side, sec_hbm, ref_hbm, sec, ref, up, down, right, left, sems):
    rows, cols = sec.shape
    copies = [
        pltpu.make_async_copy(source, target, sems.at[i])
        for i, (source, target) in enumerate([
            (sec_hbm, sec),
            (ref_hbm, ref),
            (sec_hbm.at[pl.ds(rows - pad, pad)], up.at[pl.ds(0, pad)]),
            (sec_hbm.at[pl.ds(0, pad)], down.at[pl.ds(0, pad)]),
            (ref_hbm.at[pl.ds(rows - side, side)], up.at[pl.ds(pad, side)]),
            (ref_hbm.at[pl.ds(0, side)], down.at[pl.ds(pad, side)]),
        ])
    ]
    for copy in copies:
        copy.start()
    copies[0].wait()
    copies[1].wait()
    lane = lax.broadcasted_iota(jnp.int32, (1, LANES), 1)
    right[...] = jnp.where(lane >= side, sec[:, cols - LANES:], pltpu.roll(ref[:, cols - LANES:], side, 1))
    left[...] = jnp.where(lane < LANES - side, sec[:, :LANES], pltpu.roll(ref[:, :LANES], LANES - side, 1))
    for copy in copies[2:]:
        copy.wait()


def corner_kernel(pad, left, right, up, down):
    rows = left.shape[0]
    up[:, :LANES] = left[rows - pad:]
    up[:, LANES:] = right[rows - pad:]
    down[:, :LANES] = left[:pad]
    down[:, LANES:] = right[:pad]


def main_kernel(pad, side, off_az_hbm, off_rg_hbm, slab_hbm, sec, ref, up, down, left, right, corner_up,
                corner_down, out, slab, off_az, off_rg, sec_ext, ref_ext, lhs, spec, zed, sems):
    rows, cols = sec.shape
    tiles = cols // LANES
    step = pl.program_id(0)
    width = cols + 2 * LANES
    band = cols + LANES

    def table(name):
        top, height, count, last = tables()[1][name]
        pieces = [slab[top + i * height:top + (i + 1) * height, :] for i in range(count)]
        value = jnp.concatenate(pieces, axis=1) if count > 1 else pieces[0]
        return value[:, :last]

    def twice(name):
        value = table(name)
        half = value.shape[0] // 2
        return jnp.concatenate([value[:half], value], axis=0)

    @pl.when(step == 0)
    def _():
        copies = [
            pltpu.make_async_copy(source, target, sems.at[i])
            for i, (source, target) in enumerate(
                [(slab_hbm, slab), (off_az_hbm, off_az), (off_rg_hbm, off_rg)])
        ]
        for copy in copies:
            copy.start()
        level_sec = jnp.sum(sec[...]) * (1.0 / (rows * cols))
        level_ref = jnp.sum(ref[...]) * (1.0 / (rows * cols))
        inner = slice(LANES, LANES + cols)
        sec_ext[0:pad, 0:LANES] = corner_up[:, :LANES] - level_sec
        sec_ext[0:pad, inner] = up[0:pad] - level_sec
        sec_ext[0:pad, LANES + cols:] = corner_up[:, LANES:] - level_sec
        sec_ext[pad:pad + rows, 0:LANES] = left[...] - level_sec
        sec_ext[pad:pad + rows, inner] = sec[...] - level_sec
        sec_ext[pad:pad + rows, LANES + cols:] = right[...] - level_sec
        sec_ext[pad + rows:, 0:LANES] = corner_down[:, :LANES] - level_sec
        sec_ext[pad + rows:, inner] = down[0:pad] - level_sec
        sec_ext[pad + rows:, LANES + cols:] = corner_down[:, LANES:] - level_sec
        lane = lax.broadcasted_iota(jnp.int32, (1, LANES), 1)

        def place(at, west, middle, east):
            pieces = [pltpu.roll(west, LANES - side, 1)]
            pieces += [middle[:, t * LANES:(t + 1) * LANES] for t in range(tiles)]
            pieces += [pltpu.roll(east, side, 1)]
            turned = [pltpu.roll(piece, side, 1) for piece in pieces]
            for t in range(tiles + 1):
                ref_ext[at:at + west.shape[0], t * LANES:(t + 1) * LANES] = jnp.where(
                    lane < side, turned[t], turned[t + 1]) - level_ref

        place(0, corner_up[pad - side:, :LANES], up[pad:], corner_up[pad - side:, LANES:])
        place(side, left[...], ref[...], right[...])
        place(side + rows, corner_down[:side, :LANES], down[pad:], corner_down[:side, LANES:])
        for copy in copies:
            copy.wait()

    start = step * SPACE + (pad - SPACE) + off_az[step]
    aligned = pl.multiple_of(start // 8 * 8, 8)
    field = sec_ext[pl.ds(aligned, SEARCH + 8), :]
    shift = LANES - SPACE - off_rg[step]
    turned = [pltpu.roll(field[:, t * LANES:(t + 1) * LANES], shift, 1) for t in range(tiles + 2)]
    lane = lax.broadcasted_iota(jnp.int32, (1, LANES), 1)
    field = jnp.concatenate(
        [jnp.where(lane < shift, turned[t], turned[t + 1]) for t in range(tiles + 1)], axis=1)
    field = pltpu.roll(field, SEARCH + 8 - (start - aligned), 0)[:SEARCH]
    high, low = split(field)
    spectrum = dot(table("rows_sec"), jnp.concatenate([high, low, high], axis=0))
    square_high, square_low = split(field * field)
    second = dot(table("rows_box"), jnp.concatenate([square_high, square_low], axis=0))
    first = spectrum[2 * FREQ:]
    chips = ref_ext[pl.ds(pl.multiple_of(step * SPACE, SPACE), CHIP), :]
    high, low = split(chips)
    chip_spectrum = dot(table("rows_ref"), jnp.concatenate([high, low, high], axis=0))
    count = tiles + 1
    for which, source in enumerate((spectrum, chip_spectrum)):
        for t in range(count):
            here = slice(t * LANES, (t + 1) * LANES)
            both = jnp.concatenate([source[:FREQ, here], source[FREQ:2 * FREQ, here]], axis=1)
            high, low = split(both)
            row = (which * count + t) * FREQ
            lhs[row:row + FREQ, :] = jnp.concatenate([high, low], axis=1)
    both = lhs[...]
    spec[...] = dot(jnp.concatenate([both, both[:, :2 * LANES]], axis=1), twice("columns"))

    sign = (1 - 2 * (lax.broadcasted_iota(jnp.int32, (1, LANES), 1) % 2)).astype(F32)

    def block(which, b):
        row = (which * count + b // 2) * FREQ
        base = 2 * CHIP * (b % 2)
        return spec[row:row + FREQ, base:base + CHIP], spec[row:row + FREQ, base + CHIP:base + 2 * CHIP]

    def product(b):
        (w_re, w_im), (n_re, n_im), (c_re, c_im) = block(0, b), block(0, b + 1), block(1, b)
        p_re, p_im = w_re + sign * n_re, w_im + sign * n_im
        return c_re * p_re + c_im * p_im, c_re * p_im - c_im * p_re

    chips_here = 2 * tiles
    before = product(0)
    for c in range(chips_here):
        after = product(c + 1)
        both = jnp.concatenate([before[0] + after[0], before[1] + after[1]], axis=1)
        high, low = split(both)
        row, base = (c // 2) * FREQ, 2 * CHIP * (c % 2)
        zed[row:row + FREQ, base:base + 2 * CHIP] = high
        zed[row:row + FREQ, 4 * CHIP + base:4 * CHIP + base + 2 * CHIP] = low
        before = after
    both = zed[...]
    lags = dot(jnp.concatenate([both, both[:, :4 * CHIP]], axis=1), twice("back_columns"))
    pieces = [lags[t * FREQ:(t + 1) * FREQ] for t in range(tiles)]
    stacked = jnp.concatenate(
        [jnp.concatenate([piece[:, :LANES], piece[:, LANES:]], axis=0) for piece in pieces], axis=1)
    high, low = split(stacked)
    raw = dot(table("back_rows"), jnp.concatenate([high, low, high], axis=0))

    sums = jnp.concatenate([first, second], axis=0)
    sums = jnp.concatenate([sums[:, t * LANES:(t + 2) * LANES] for t in range(tiles)], axis=0)
    high, low = split(sums)
    boxes = dot(jnp.concatenate([high, low], axis=1), jnp.concatenate([table("slide")] * 2, axis=0))
    totals = jnp.concatenate(
        [jnp.sum(chips.reshape(CHIP // 8, 8, band), axis=0),
         jnp.sum((chips * chips).reshape(CHIP // 8, 8, band), axis=0)], axis=0)
    totals = jnp.concatenate([totals[:, t * LANES:(t + 2) * LANES] for t in range(tiles)], axis=0)
    high, low = split(totals)
    rest = (totals - high.astype(F32) - low.astype(F32)).astype(BF16)
    totals = dot(jnp.concatenate([high, low, rest], axis=1), jnp.concatenate([table("gather")] * 3, axis=0))

    scores = []
    for t in range(tiles):
        first_t = boxes[t * CHIP:t * CHIP + LAGS]
        second_t = boxes[t * CHIP + LAGS:(t + 1) * CHIP]
        total = jnp.sum(totals[16 * t:16 * t + 8], axis=0, keepdims=True)
        power = jnp.sum(totals[16 * t + 8:16 * t + 16], axis=0, keepdims=True)
        corr = raw[:, t * LANES:(t + 1) * LANES] - (total * (1.0 / AREA)) * first_t
        var_sum = second_t - first_t * first_t * (1.0 / AREA)
        energy = power - total * total * (1.0 / AREA)
        scores.append(CHIP * (corr * (1.0 / AREA)) * lax.rsqrt(
            (energy * (1.0 / AREA)) * (var_sum * (1.0 / AREA)) + EPSILON))
    high, low = split(jnp.concatenate(scores, axis=1))
    lifted = dot(table("cubic_rows"), jnp.concatenate([high, low], axis=0))
    lifted = jnp.concatenate([lifted[:, t * LANES:(t + 1) * LANES] for t in range(tiles)], axis=0)
    high, low = split(lifted)
    fine = dot(jnp.concatenate([high, low], axis=1), jnp.concatenate([table("cubic_cols")] * 2, axis=0))
    for c in range(chips_here):
        row, base = (c // 2) * CHIP, CHIP * (c % 2)
        out[0, c] = fine[row:row + CHIP, base:base + CHIP]


def neighbours(axis):
    size = lax.axis_size(axis)
    forth = [(i, i + 1) for i in range(size - 1)]
    return forth, [(j, i) for i, j in forth]


def body(ref_image, sec_image, off_az, off_rg):
    rows, cols = ref_image.shape
    side = CHIP // 4
    chip_rows, chip_cols = rows // SPACE, cols // SPACE
    all_rows = chip_rows * lax.axis_size("az")
    reach = min(SPACE - 1, (all_rows - 1) // 2)
    pad = -(-(SPACE + reach) // 8) * 8
    assert SPACE + reach + side <= LANES
    tiles = cols // LANES

    tall = rows + 2 * pad

    def full(*shape):
        return jax.ShapeDtypeStruct(shape, F32)

    away = pl.BlockSpec(memory_space=pltpu.MemorySpace.HBM)
    sec, ref, to_up, to_down, to_right, to_left = pl.pallas_call(
        functools.partial(pack_kernel, pad, side),
        in_specs=[away] * 2,
        out_shape=[full(rows, cols)] * 2 + [full(pad + side, cols)] * 2 + [full(rows, LANES)] * 2,
        scratch_shapes=[pltpu.SemaphoreType.DMA((6,))],
        compiler_params=pltpu.CompilerParams(vmem_limit_bytes=8 << 20),
    )(*(pltpu.with_memory_space_constraint(x, pltpu.MemorySpace.HBM) for x in (sec_image, ref_image)))
    forth, back = neighbours("az")
    east, west = neighbours("rg")
    up = lax.ppermute(to_up, "az", forth)
    down = lax.ppermute(to_down, "az", back)
    left = lax.ppermute(to_right, "rg", east)
    right = lax.ppermute(to_left, "rg", west)
    corners_up, corners_down = pl.pallas_call(
        functools.partial(corner_kernel, pad),
        out_shape=[full(pad, 2 * LANES)] * 2,
        compiler_params=pltpu.CompilerParams(vmem_limit_bytes=8 << 20),
    )(left, right)
    corner_up = lax.ppermute(corners_up, "az", forth)
    corner_down = lax.ppermute(corners_down, "az", back)

    slab = jnp.asarray(tables()[0])
    operands = [sec, ref, up, down, left, right, corner_up, corner_down]
    count = tiles + 1

    def whole(x):
        return pl.BlockSpec(x.shape, lambda i: (0, 0), pipeline_mode=pl.Buffered(1))

    return pl.pallas_call(
        functools.partial(main_kernel, pad, side),
        grid=(chip_rows,),
        in_specs=[away] * 3 + [whole(x) for x in operands],
        out_specs=pl.BlockSpec((1, chip_cols, 2 * LAGS, 2 * LAGS), lambda i: (i, 0, 0, 0)),
        scratch_shapes=[
            pltpu.VMEM(slab.shape, BF16),
            pltpu.SMEM((chip_rows,), jnp.int32),
            pltpu.SMEM((chip_rows,), jnp.int32),
            pltpu.VMEM((tall, cols + 2 * LANES), F32),
            pltpu.VMEM((rows + 2 * side, cols + LANES), F32),
            pltpu.VMEM((2 * count * FREQ, 4 * LANES), BF16),
            pltpu.VMEM((2 * count * FREQ, 4 * CHIP), F32),
            pltpu.VMEM((tiles * FREQ, 8 * CHIP), BF16),
            pltpu.SemaphoreType.DMA((3,)),
        ],
        out_shape=full(chip_rows, chip_cols, 2 * LAGS, 2 * LAGS),
        compiler_params=pltpu.CompilerParams(dimension_semantics=("arbitrary",), vmem_limit_bytes=40 << 20),
    )(*(pltpu.with_memory_space_constraint(x, pltpu.MemorySpace.HBM) for x in (off_az, off_rg, slab)), *operands)


def solution(mesh):
    return jax.shard_map(
        body,
        mesh=mesh,
        in_specs=(P("az", "rg"), P("az", "rg"), P("az"), P("az")),
        out_specs=P("az", "rg", None, None),
        check_vma=False,
    )
```

```python
import functools
import math

import jax
import jax.numpy as jnp
import numpy as np
from jax import lax
from jax.experimental import pallas as pl
from jax.experimental.pallas import tpu as pltpu
from jax.sharding import PartitionSpec as P


CHIP = 128
SPACE = 64
SEARCH = 192
LAGS = 64
LANES = 128
FREQ = SEARCH // 2
EPSILON = 1e-06
AREA = float(CHIP * CHIP)
BF16 = jnp.bfloat16
F32 = jnp.float32


def halves(table):
    high = table.astype(BF16)
    low = (table - high.astype(np.float64)).astype(BF16)
    return high, low


@functools.cache
def tables():
    theta = 2.0 * math.pi * (np.arange(FREQ)[:, None] + 0.5) / SEARCH
    cell = np.arange(SEARCH)[None, :]
    forward = np.concatenate([np.cos(theta * cell), -np.sin(theta * cell)], axis=0)
    lag = np.arange(LAGS)[:, None]
    box = ((cell >= lag) & (cell < lag + CHIP)).astype(np.float64)
    made = {}
    high, low = halves(np.concatenate([forward, box], axis=0))
    made["rows_sec"] = np.concatenate([high, high, low], axis=1)
    high, low = halves(forward[:, :CHIP])
    made["rows_ref"] = np.concatenate([high, high, low], axis=1)
    made["rows_box"] = np.concatenate([box, box], axis=1).astype(BF16)

    phi = 2.0 * math.pi / CHIP * np.arange(CHIP)[None, :]
    spot = np.arange(SPACE)[:, None]
    cosine, sine = np.cos(phi * spot), np.sin(phi * spot)
    parts = (np.concatenate([cosine, -sine], axis=1), np.concatenate([sine, cosine], axis=1))
    made["columns"] = np.concatenate(halves(np.concatenate(parts, axis=0)), axis=0)

    cosine, sine = np.cos(phi.T * lag.T), np.sin(phi.T * lag.T)
    back = np.concatenate(
        [np.concatenate([cosine, sine], axis=1), np.concatenate([-sine, cosine], axis=1)], axis=0)
    made["back_columns"] = np.concatenate(halves(back), axis=1)

    final = np.concatenate([np.cos(theta.T * lag), -np.sin(theta.T * lag)], axis=1)
    high, low = halves(final * (2.0 / (SEARCH * CHIP)))
    made["back_rows"] = np.concatenate([high, high, low], axis=1)

    wide = np.arange(2 * LANES)[:, None]
    lane = np.arange(LANES)[None, :]
    start = lane // SPACE * SPACE
    made["slide"] = ((wide >= lane) & (wide < lane + CHIP)).astype(BF16)
    made["gather"] = ((wide >= start) & (wide < start + CHIP)).astype(BF16)

    out_index = np.arange(2 * LAGS)[:, None]
    sample = np.arange(LAGS)[None, :]
    base = out_index // 2

    def pick(where):
        return (np.clip(where, 0, LAGS - 1) == sample).astype(np.float64)

    odd = (9.0 * (pick(base) + pick(base + 1)) - (pick(base - 1) + pick(base + 2))) / 16.0
    cubic = np.where(out_index % 2 == 1, odd, pick(base))
    made["cubic_rows"] = np.concatenate([cubic, cubic], axis=1).astype(BF16)
    zero = np.zeros_like(cubic.T)
    made["cubic_cols"] = np.concatenate(
        [np.concatenate([cubic.T, zero], axis=1), np.concatenate([zero, cubic.T], axis=1)], axis=0
    ).astype(BF16)

    slabs, places, top = [], {}, 0
    for name, table in made.items():
        table = np.pad(table, ((0, 0), (0, -table.shape[1] % LANES)))
        pieces = [table[:, i:i + LANES] for i in range(0, table.shape[1], LANES)]
        places[name] = (top, table.shape[0], len(pieces), made[name].shape[1])
        slabs += pieces
        top += table.shape[0] * len(pieces)
    return np.concatenate(slabs, axis=0), places


def split(value):
    high = value.astype(BF16)
    low = (value - high.astype(F32)).astype(BF16)
    return high, low


def dot(left, right):
    return jnp.dot(left, right, preferred_element_type=F32)


def pack_kernel(pad, side, sec_hbm, ref_hbm, sec, ref, up, down, right, left, sems):
    rows, cols = sec.shape
    copies = [
        pltpu.make_async_copy(source, target, sems.at[i])
        for i, (source, target) in enumerate([
            (sec_hbm, sec),
            (ref_hbm, ref),
            (sec_hbm.at[pl.ds(rows - pad, pad)], up.at[pl.ds(0, pad)]),
            (sec_hbm.at[pl.ds(0, pad)], down.at[pl.ds(0, pad)]),
            (ref_hbm.at[pl.ds(rows - side, side)], up.at[pl.ds(pad, side)]),
            (ref_hbm.at[pl.ds(0, side)], down.at[pl.ds(pad, side)]),
        ])
    ]
    for copy in copies:
        copy.start()
    copies[0].wait()
    copies[1].wait()
    lane = lax.broadcasted_iota(jnp.int32, (1, LANES), 1)
    right[...] = jnp.where(lane >= side, sec[:, cols - LANES:], pltpu.roll(ref[:, cols - LANES:], side, 1))
    left[...] = jnp.where(lane < LANES - side, sec[:, :LANES], pltpu.roll(ref[:, :LANES], LANES - side, 1))
    for copy in copies[2:]:
        copy.wait()


def corner_kernel(pad, left, right, up, down):
    rows = left.shape[0]
    up[:, :LANES] = left[rows - pad:]
    up[:, LANES:] = right[rows - pad:]
    down[:, :LANES] = left[:pad]
    down[:, LANES:] = right[:pad]


def main_kernel(pad, side, off_az_hbm, off_rg_hbm, slab_hbm, sec, ref, up, down, left, right, corner_up,
                corner_down, out, slab, off_az, off_rg, sec_ext, ref_ext, lhs, spec, zed, sems):
    rows, cols = sec.shape
    tiles = cols // LANES
    step = pl.program_id(0)
    band = cols + LANES

    def table(name):
        top, height, count, last = tables()[1][name]
        pieces = [slab[top + i * height:top + (i + 1) * height, :] for i in range(count)]
        value = jnp.concatenate(pieces, axis=1) if count > 1 else pieces[0]
        return value[:, :last]

    @pl.when(step == 0)
    def _():
        copies = [
            pltpu.make_async_copy(source, target, sems.at[i])
            for i, (source, target) in enumerate(
                [(slab_hbm, slab), (off_az_hbm, off_az), (off_rg_hbm, off_rg)])
        ]
        for copy in copies:
            copy.start()
        level_sec = jnp.sum(sec[...]) * (1.0 / (rows * cols))
        level_ref = jnp.sum(ref[...]) * (1.0 / (rows * cols))
        inner = slice(LANES, LANES + cols)
        sec_ext[0:pad, 0:LANES] = corner_up[:, :LANES] - level_sec
        sec_ext[0:pad, inner] = up[0:pad] - level_sec
        sec_ext[0:pad, LANES + cols:] = corner_up[:, LANES:] - level_sec
        sec_ext[pad:pad + rows, 0:LANES] = left[...] - level_sec
        sec_ext[pad:pad + rows, inner] = sec[...] - level_sec
        sec_ext[pad:pad + rows, LANES + cols:] = right[...] - level_sec
        sec_ext[pad + rows:, 0:LANES] = corner_down[:, :LANES] - level_sec
        sec_ext[pad + rows:, inner] = down[0:pad] - level_sec
        sec_ext[pad + rows:, LANES + cols:] = corner_down[:, LANES:] - level_sec
        lane = lax.broadcasted_iota(jnp.int32, (1, LANES), 1)

        def place(at, west, middle, east):
            pieces = [pltpu.roll(west, LANES - side, 1)]
            pieces += [middle[:, t * LANES:(t + 1) * LANES] for t in range(tiles)]
            pieces += [pltpu.roll(east, side, 1)]
            turned = [pltpu.roll(piece, side, 1) for piece in pieces]
            for t in range(tiles + 1):
                ref_ext[at:at + west.shape[0], t * LANES:(t + 1) * LANES] = jnp.where(
                    lane < side, turned[t], turned[t + 1]) - level_ref

        place(0, corner_up[pad - side:, :LANES], up[pad:], corner_up[pad - side:, LANES:])
        place(side, left[...], ref[...], right[...])
        place(side + rows, corner_down[:side, :LANES], down[pad:], corner_down[:side, LANES:])
        for copy in copies:
            copy.wait()

    count = tiles + 1

    lane = lax.broadcasted_iota(jnp.int32, (1, LANES), 1)
    both = table("columns")
    major, minor = jnp.concatenate([both[:LANES]] * 2, axis=0), both[LANES:]

    def spread(which, source):
        for t in range(count):
            here = slice(t * LANES, (t + 1) * LANES)
            real, imag = source[:FREQ, here], source[FREQ:2 * FREQ, here]
            even = jnp.where(lane < SPACE, real, pltpu.roll(imag, SPACE, 1))
            odd = jnp.where(lane < SPACE, pltpu.roll(real, SPACE, 1), imag)
            for i, value in enumerate((even, odd)):
                row = ((which * count + t) * 2 + i) * FREQ
                lhs[row:row + FREQ, :] = jnp.concatenate(split(value), axis=1)
        for i in range(2):
            low = (which * 2 + i) * count * FREQ
            here = slice(low, low + count * FREQ)
            spec[here, :] = dot(lhs[here, :], major) + dot(lhs[here, :LANES], minor)

    chips = ref_ext[pl.ds(pl.multiple_of(step * SPACE, SPACE), CHIP), :]
    high, low = split(chips)
    spread(1, dot(table("rows_ref"), jnp.concatenate([high, low, high], axis=0)))

    start = step * SPACE + (pad - SPACE) + off_az[step]
    aligned = pl.multiple_of(start // 8 * 8, 8)
    field = sec_ext[pl.ds(aligned, SEARCH + 8), :]
    shift = LANES - SPACE - off_rg[step]
    turned = [pltpu.roll(field[:, t * LANES:(t + 1) * LANES], shift, 1) for t in range(tiles + 2)]
    lane = lax.broadcasted_iota(jnp.int32, (1, LANES), 1)
    field = jnp.concatenate(
        [jnp.where(lane < shift, turned[t], turned[t + 1]) for t in range(tiles + 1)], axis=1)
    part = start - aligned
    field = pltpu.roll(field.reshape(SEARCH // 8 + 1, 8, band), 8 - part, 1)
    line = lax.broadcasted_iota(jnp.int32, (1, 8, 1), 1)
    field = jnp.where(line < 8 - part, field[:-1], field[1:]).reshape(SEARCH, band)
    high, low = split(field)
    spectrum = dot(table("rows_sec"), jnp.concatenate([high, low, high], axis=0))
    square_high, square_low = split(field * field)
    second = dot(table("rows_box"), jnp.concatenate([square_high, square_low], axis=0))
    first = spectrum[2 * FREQ:]
    spread(0, spectrum)

    sign = (1 - 2 * (lax.broadcasted_iota(jnp.int32, (1, LANES), 1) % 2)).astype(F32)

    def block(which, b):
        row = (which * count * 2 + b) * FREQ
        return spec[row:row + FREQ, :CHIP], spec[row:row + FREQ, CHIP:]

    def product(b):
        (w_re, w_im), (n_re, n_im), (c_re, c_im) = block(0, b), block(0, b + 1), block(1, b)
        p_re, p_im = w_re + sign * n_re, w_im + sign * n_im
        return c_re * p_re + c_im * p_im, c_re * p_im - c_im * p_re

    chips_here = 2 * tiles
    before = product(0)
    for c in range(chips_here):
        after = product(c + 1)
        both = jnp.concatenate([before[0] + after[0], before[1] + after[1]], axis=1)
        high, low = split(both)
        row = c * FREQ
        zed[row:row + FREQ, :2 * CHIP] = high
        zed[row:row + FREQ, 2 * CHIP:] = low
        before = after
    back = table("back_columns")
    main = dot(zed[:, :2 * CHIP], back)
    rest = dot(zed[:, 2 * CHIP:], back[:, :2 * LAGS])
    pieces = []
    for t in range(tiles):
        pair = []
        for row in (2 * t * FREQ, (2 * t + 1) * FREQ):
            here = main[row:row + FREQ]
            pair.append(here[:, :LANES] + here[:, LANES:] + rest[row:row + FREQ])
        even, odd = pair[0], pair[1]
        odd_turned, even_turned = pltpu.roll(odd, LAGS, 1), pltpu.roll(even, LAGS, 1)
        pieces.append(jnp.concatenate(
            [jnp.where(lane < LAGS, even, odd_turned), jnp.where(lane < LAGS, even_turned, odd)], axis=0))
    stacked = jnp.concatenate(pieces, axis=1)
    high, low = split(stacked)
    raw = dot(table("back_rows"), jnp.concatenate([high, low, high], axis=0))

    slide = jnp.concatenate([table("slide")] * 2, axis=0)

    def boxes(sums):
        sums = jnp.concatenate([sums[:, t * LANES:(t + 2) * LANES] for t in range(tiles)], axis=0)
        return dot(jnp.concatenate(split(sums), axis=1), slide)

    firsts, seconds = boxes(first), boxes(second)
    totals = jnp.concatenate(
        [jnp.sum(chips.reshape(CHIP // 8, 8, band), axis=0),
         jnp.sum((chips * chips).reshape(CHIP // 8, 8, band), axis=0)], axis=0)
    totals = jnp.concatenate([totals[:, t * LANES:(t + 2) * LANES] for t in range(tiles)], axis=0)
    high, low = split(totals)
    rest = (totals - high.astype(F32) - low.astype(F32)).astype(BF16)
    totals = dot(jnp.concatenate([high, low, rest], axis=1), jnp.concatenate([table("gather")] * 3, axis=0))

    scores = []
    for t in range(tiles):
        first_t = firsts[t * LAGS:(t + 1) * LAGS]
        second_t = seconds[t * LAGS:(t + 1) * LAGS]
        total = jnp.sum(totals[16 * t:16 * t + 8], axis=0, keepdims=True)
        power = jnp.sum(totals[16 * t + 8:16 * t + 16], axis=0, keepdims=True)
        corr = raw[:, t * LANES:(t + 1) * LANES] - (total * (1.0 / AREA)) * first_t
        var_sum = second_t - first_t * first_t * (1.0 / AREA)
        energy = power - total * total * (1.0 / AREA)
        scores.append(CHIP * (corr * (1.0 / AREA)) * lax.rsqrt(
            (energy * (1.0 / AREA)) * (var_sum * (1.0 / AREA)) + EPSILON))
    high, low = split(jnp.concatenate(scores, axis=1))
    lifted = dot(table("cubic_rows"), jnp.concatenate([high, low], axis=0))
    cubic = jnp.concatenate([table("cubic_cols")] * 2, axis=0)
    half = (tiles + 1) // 2
    for begin, end in ((0, half), (half, tiles)):
        part = jnp.concatenate([lifted[:, t * LANES:(t + 1) * LANES] for t in range(begin, end)], axis=0)
        fine = dot(jnp.concatenate(split(part), axis=1), cubic)
        for t in range(begin, end):
            row = (t - begin) * CHIP
            out[0, 2 * t] = fine[row:row + CHIP, :CHIP]
            out[0, 2 * t + 1] = fine[row:row + CHIP, CHIP:]


def neighbours(axis):
    size = lax.axis_size(axis)
    forth = [(i, i + 1) for i in range(size - 1)]
    return forth, [(j, i) for i, j in forth]


def body(ref_image, sec_image, off_az, off_rg):
    rows, cols = ref_image.shape
    side = CHIP // 4
    chip_rows, chip_cols = rows // SPACE, cols // SPACE
    all_rows = chip_rows * lax.axis_size("az")
    reach = min(SPACE - 1, (all_rows - 1) // 2)
    pad = -(-(SPACE + reach) // 8) * 8
    assert SPACE + reach + side <= LANES
    tiles = cols // LANES

    tall = rows + 2 * pad

    def full(*shape):
        return jax.ShapeDtypeStruct(shape, F32)

    away = pl.BlockSpec(memory_space=pltpu.MemorySpace.HBM)
    sec, ref, to_up, to_down, to_right, to_left = pl.pallas_call(
        functools.partial(pack_kernel, pad, side),
        in_specs=[away] * 2,
        out_shape=[full(rows, cols)] * 2 + [full(pad + side, cols)] * 2 + [full(rows, LANES)] * 2,
        scratch_shapes=[pltpu.SemaphoreType.DMA((6,))],
        compiler_params=pltpu.CompilerParams(vmem_limit_bytes=8 << 20),
    )(*(pltpu.with_memory_space_constraint(x, pltpu.MemorySpace.HBM) for x in (sec_image, ref_image)))
    forth, back = neighbours("az")
    east, west = neighbours("rg")
    up = lax.ppermute(to_up, "az", forth)
    down = lax.ppermute(to_down, "az", back)
    left = lax.ppermute(to_right, "rg", east)
    right = lax.ppermute(to_left, "rg", west)
    corners_up, corners_down = pl.pallas_call(
        functools.partial(corner_kernel, pad),
        out_shape=[full(pad, 2 * LANES)] * 2,
        compiler_params=pltpu.CompilerParams(vmem_limit_bytes=8 << 20),
    )(left, right)
    corner_up = lax.ppermute(corners_up, "az", forth)
    corner_down = lax.ppermute(corners_down, "az", back)

    slab = jnp.asarray(tables()[0])
    operands = [sec, ref, up, down, left, right, corner_up, corner_down]
    count = tiles + 1

    def whole(x):
        return pl.BlockSpec(x.shape, lambda i: (0, 0), pipeline_mode=pl.Buffered(1))

    return pl.pallas_call(
        functools.partial(main_kernel, pad, side),
        grid=(chip_rows,),
        in_specs=[away] * 3 + [whole(x) for x in operands],
        out_specs=pl.BlockSpec((1, chip_cols, 2 * LAGS, 2 * LAGS), lambda i: (i, 0, 0, 0)),
        scratch_shapes=[
            pltpu.VMEM(slab.shape, BF16),
            pltpu.SMEM((chip_rows,), jnp.int32),
            pltpu.SMEM((chip_rows,), jnp.int32),
            pltpu.VMEM((tall, cols + 2 * LANES), F32),
            pltpu.VMEM((rows + 2 * side, cols + LANES), F32),
            pltpu.VMEM((4 * count * FREQ, 2 * LANES), BF16),
            pltpu.VMEM((4 * count * FREQ, 2 * CHIP), F32),
            pltpu.VMEM((chip_cols * FREQ, 4 * CHIP), BF16),
            pltpu.SemaphoreType.DMA((3,)),
        ],
        out_shape=full(chip_rows, chip_cols, 2 * LAGS, 2 * LAGS),
        compiler_params=pltpu.CompilerParams(dimension_semantics=("arbitrary",), vmem_limit_bytes=40 << 20),
    )(*(pltpu.with_memory_space_constraint(x, pltpu.MemorySpace.HBM) for x in (off_az, off_rg, slab)), *operands)


def solution(mesh):
    return jax.shard_map(
        body,
        mesh=mesh,
        in_specs=(P("az", "rg"), P("az", "rg"), P("az"), P("az")),
        out_specs=P("az", "rg", None, None),
        check_vma=False,
    )
```

```python
import functools
import math

import jax
import jax.numpy as jnp
import numpy as np
from jax import lax
from jax.experimental import pallas as pl
from jax.experimental.pallas import tpu as pltpu
from jax.sharding import PartitionSpec as P


CHIP = 128
SPACE = 64
SEARCH = 192
LAGS = 64
LANES = 128
FREQ = SEARCH // 2
EPSILON = 1e-06
AREA = float(CHIP * CHIP)
BF16 = jnp.bfloat16
F32 = jnp.float32


def halves(table):
    high = table.astype(BF16)
    low = (table - high.astype(np.float64)).astype(BF16)
    return high, low


@functools.cache
def tables():
    theta = 2.0 * math.pi * (np.arange(FREQ)[:, None] + 0.5) / SEARCH
    cell = np.arange(SEARCH)[None, :]
    forward = np.concatenate([np.cos(theta * cell), -np.sin(theta * cell)], axis=0)
    lag = np.arange(LAGS)[:, None]
    box = ((cell >= lag) & (cell < lag + CHIP)).astype(np.float64)
    made = {}
    high, low = halves(np.concatenate([forward, box], axis=0))
    made["rows_sec"] = np.concatenate([high, high, low], axis=1)
    high, low = halves(forward[:, :CHIP])
    made["rows_ref"] = np.concatenate([high, high, low], axis=1)
    made["rows_box"] = np.concatenate([box, box], axis=1).astype(BF16)

    phi = 2.0 * math.pi / CHIP * np.arange(CHIP)[None, :]
    spot = np.arange(SPACE)[:, None]
    cosine, sine = np.cos(phi * spot), np.sin(phi * spot)
    parts = (np.concatenate([cosine, -sine], axis=1), np.concatenate([sine, cosine], axis=1))
    made["columns"] = np.concatenate(halves(np.concatenate(parts, axis=0)), axis=0)

    cosine, sine = np.cos(phi.T * lag.T), np.sin(phi.T * lag.T)
    back = np.concatenate(
        [np.concatenate([cosine, sine], axis=1), np.concatenate([-sine, cosine], axis=1)], axis=0)
    made["back_columns"] = np.concatenate(halves(back), axis=1)

    final = np.concatenate([np.cos(theta.T * lag), -np.sin(theta.T * lag)], axis=1)
    high, low = halves(final * (2.0 / (SEARCH * CHIP)))
    made["back_rows"] = np.concatenate([high, high, low], axis=1)

    wide = np.arange(2 * LANES)[:, None]
    lane = np.arange(LANES)[None, :]
    start = lane // SPACE * SPACE
    made["slide"] = ((wide >= lane) & (wide < lane + CHIP)).astype(BF16)
    made["gather"] = ((wide >= start) & (wide < start + CHIP)).astype(BF16)

    out_index = np.arange(2 * LAGS)[:, None]
    sample = np.arange(LAGS)[None, :]
    base = out_index // 2

    def pick(where):
        return (np.clip(where, 0, LAGS - 1) == sample).astype(np.float64)

    odd = (9.0 * (pick(base) + pick(base + 1)) - (pick(base - 1) + pick(base + 2))) / 16.0
    cubic = np.where(out_index % 2 == 1, odd, pick(base))
    made["cubic_rows"] = np.concatenate([cubic, cubic], axis=1).astype(BF16)
    zero = np.zeros_like(cubic.T)
    made["cubic_cols"] = np.concatenate(
        [np.concatenate([cubic.T, zero], axis=1), np.concatenate([zero, cubic.T], axis=1)], axis=0
    ).astype(BF16)

    slabs, places, top = [], {}, 0
    for name, table in made.items():
        table = np.pad(table, ((0, 0), (0, -table.shape[1] % LANES)))
        pieces = [table[:, i:i + LANES] for i in range(0, table.shape[1], LANES)]
        places[name] = (top, table.shape[0], len(pieces), made[name].shape[1])
        slabs += pieces
        top += table.shape[0] * len(pieces)
    return np.concatenate(slabs, axis=0), places


def split(value):
    high = value.astype(BF16)
    low = (value - high.astype(F32)).astype(BF16)
    return high, low


def dot(left, right):
    return jnp.dot(left, right, preferred_element_type=F32)


def pack_kernel(pad, side, sec_hbm, ref_hbm, sec, ref, up, down, right, left, sems):
    rows, cols = sec.shape
    copies = [
        pltpu.make_async_copy(source, target, sems.at[i])
        for i, (source, target) in enumerate([
            (sec_hbm, sec),
            (ref_hbm, ref),
            (sec_hbm.at[pl.ds(rows - pad, pad)], up.at[pl.ds(0, pad)]),
            (sec_hbm.at[pl.ds(0, pad)], down.at[pl.ds(0, pad)]),
            (ref_hbm.at[pl.ds(rows - side, side)], up.at[pl.ds(pad, side)]),
            (ref_hbm.at[pl.ds(0, side)], down.at[pl.ds(pad, side)]),
        ])
    ]
    for copy in copies:
        copy.start()
    copies[0].wait()
    copies[1].wait()
    lane = lax.broadcasted_iota(jnp.int32, (1, LANES), 1)
    right[...] = jnp.where(lane >= side, sec[:, cols - LANES:], pltpu.roll(ref[:, cols - LANES:], side, 1))
    left[...] = jnp.where(lane < LANES - side, sec[:, :LANES], pltpu.roll(ref[:, :LANES], LANES - side, 1))
    for copy in copies[2:]:
        copy.wait()


def corner_kernel(pad, left, right, up, down):
    rows = left.shape[0]
    up[:, :LANES] = left[rows - pad:]
    up[:, LANES:] = right[rows - pad:]
    down[:, :LANES] = left[:pad]
    down[:, LANES:] = right[:pad]


def fetch_kernel(source, target, sem):
    copy = pltpu.make_async_copy(source, target, sem)
    copy.start()
    copy.wait()


def main_kernel(pad, side, off_az_hbm, off_rg_hbm, slab, sec, ref, up, down, left, right, corner_up,
                corner_down, out, off_az, off_rg, sec_ext, ref_ext, lhs, spec, zed, sems):
    rows, cols = sec.shape
    tiles = cols // LANES
    step = pl.program_id(0)
    band = cols + LANES

    def table(name):
        top, height, count, last = tables()[1][name]
        pieces = [slab[top + i * height:top + (i + 1) * height, :] for i in range(count)]
        value = jnp.concatenate(pieces, axis=1) if count > 1 else pieces[0]
        return value[:, :last]

    @pl.when(step == 0)
    def _():
        copies = [
            pltpu.make_async_copy(source, target, sems.at[i])
            for i, (source, target) in enumerate(
                [(off_az_hbm, off_az), (off_rg_hbm, off_rg)])
        ]
        for copy in copies:
            copy.start()
        level_sec = jnp.sum(sec[...]) * (1.0 / (rows * cols))
        level_ref = jnp.sum(ref[...]) * (1.0 / (rows * cols))
        inner = slice(LANES, LANES + cols)
        sec_ext[0:pad, 0:LANES] = corner_up[:, :LANES] - level_sec
        sec_ext[0:pad, inner] = up[0:pad] - level_sec
        sec_ext[0:pad, LANES + cols:] = corner_up[:, LANES:] - level_sec
        sec_ext[pad:pad + rows, 0:LANES] = left[...] - level_sec
        sec_ext[pad:pad + rows, inner] = sec[...] - level_sec
        sec_ext[pad:pad + rows, LANES + cols:] = right[...] - level_sec
        sec_ext[pad + rows:, 0:LANES] = corner_down[:, :LANES] - level_sec
        sec_ext[pad + rows:, inner] = down[0:pad] - level_sec
        sec_ext[pad + rows:, LANES + cols:] = corner_down[:, LANES:] - level_sec
        lane = lax.broadcasted_iota(jnp.int32, (1, LANES), 1)

        def place(at, west, middle, east):
            pieces = [pltpu.roll(west, LANES - side, 1)]
            pieces += [middle[:, t * LANES:(t + 1) * LANES] for t in range(tiles)]
            pieces += [pltpu.roll(east, side, 1)]
            turned = [pltpu.roll(piece, side, 1) for piece in pieces]
            for t in range(tiles + 1):
                ref_ext[at:at + west.shape[0], t * LANES:(t + 1) * LANES] = jnp.where(
                    lane < side, turned[t], turned[t + 1]) - level_ref

        place(0, corner_up[pad - side:, :LANES], up[pad:], corner_up[pad - side:, LANES:])
        place(side, left[...], ref[...], right[...])
        place(side + rows, corner_down[:side, :LANES], down[pad:], corner_down[:side, LANES:])
        for copy in copies:
            copy.wait()

    count = tiles + 1

    lane = lax.broadcasted_iota(jnp.int32, (1, LANES), 1)
    both = table("columns")
    major, minor = jnp.concatenate([both[:LANES]] * 2, axis=0), both[LANES:]

    def spread(which, source):
        for t in range(count):
            here = slice(t * LANES, (t + 1) * LANES)
            real, imag = source[:FREQ, here], source[FREQ:2 * FREQ, here]
            even = jnp.where(lane < SPACE, real, pltpu.roll(imag, SPACE, 1))
            odd = jnp.where(lane < SPACE, pltpu.roll(real, SPACE, 1), imag)
            for i, value in enumerate((even, odd)):
                row = ((which * count + t) * 2 + i) * FREQ
                lhs[row:row + FREQ, :] = jnp.concatenate(split(value), axis=1)
        for i in range(2):
            low = (which * 2 + i) * count * FREQ
            here = slice(low, low + count * FREQ)
            spec[here, :] = dot(lhs[here, :], major) + dot(lhs[here, :LANES], minor)

    chips = ref_ext[pl.ds(pl.multiple_of(step * SPACE, SPACE), CHIP), :]
    high, low = split(chips)
    spread(1, dot(table("rows_ref"), jnp.concatenate([high, low, high], axis=0)))

    start = step * SPACE + (pad - SPACE) + off_az[step]
    aligned = pl.multiple_of(start // 8 * 8, 8)
    field = sec_ext[pl.ds(aligned, SEARCH + 8), :]
    shift = LANES - SPACE - off_rg[step]
    turned = [pltpu.roll(field[:, t * LANES:(t + 1) * LANES], shift, 1) for t in range(tiles + 2)]
    lane = lax.broadcasted_iota(jnp.int32, (1, LANES), 1)
    field = jnp.concatenate(
        [jnp.where(lane < shift, turned[t], turned[t + 1]) for t in range(tiles + 1)], axis=1)
    part = start - aligned
    field = pltpu.roll(field.reshape(SEARCH // 8 + 1, 8, band), 8 - part, 1)
    line = lax.broadcasted_iota(jnp.int32, (1, 8, 1), 1)
    field = jnp.where(line < 8 - part, field[:-1], field[1:]).reshape(SEARCH, band)
    high, low = split(field)
    spectrum = dot(table("rows_sec"), jnp.concatenate([high, low, high], axis=0))
    square_high, square_low = split(field * field)
    second = dot(table("rows_box"), jnp.concatenate([square_high, square_low], axis=0))
    first = spectrum[2 * FREQ:]
    spread(0, spectrum)

    sign = (1 - 2 * (lax.broadcasted_iota(jnp.int32, (1, LANES), 1) % 2)).astype(F32)

    def block(which, b):
        row = (which * count * 2 + b) * FREQ
        return spec[row:row + FREQ, :CHIP], spec[row:row + FREQ, CHIP:]

    def product(b):
        (w_re, w_im), (n_re, n_im), (c_re, c_im) = block(0, b), block(0, b + 1), block(1, b)
        p_re, p_im = w_re + sign * n_re, w_im + sign * n_im
        return c_re * p_re + c_im * p_im, c_re * p_im - c_im * p_re

    chips_here = 2 * tiles
    before = product(0)
    for c in range(chips_here):
        after = product(c + 1)
        both = jnp.concatenate([before[0] + after[0], before[1] + after[1]], axis=1)
        high, low = split(both)
        row = c * FREQ
        zed[row:row + FREQ, :2 * CHIP] = high
        zed[row:row + FREQ, 2 * CHIP:] = low
        before = after
    back = table("back_columns")
    main = dot(zed[:, :2 * CHIP], back)
    rest = dot(zed[:, 2 * CHIP:], back[:, :2 * LAGS])
    pieces = []
    for t in range(tiles):
        pair = []
        for row in (2 * t * FREQ, (2 * t + 1) * FREQ):
            here = main[row:row + FREQ]
            pair.append(here[:, :LANES] + here[:, LANES:] + rest[row:row + FREQ])
        even, odd = pair[0], pair[1]
        odd_turned, even_turned = pltpu.roll(odd, LAGS, 1), pltpu.roll(even, LAGS, 1)
        pieces.append(jnp.concatenate(
            [jnp.where(lane < LAGS, even, odd_turned), jnp.where(lane < LAGS, even_turned, odd)], axis=0))
    stacked = jnp.concatenate(pieces, axis=1)
    high, low = split(stacked)
    raw = dot(table("back_rows"), jnp.concatenate([high, low, high], axis=0))

    slide = jnp.concatenate([table("slide")] * 2, axis=0)

    def boxes(sums):
        sums = jnp.concatenate([sums[:, t * LANES:(t + 2) * LANES] for t in range(tiles)], axis=0)
        return dot(jnp.concatenate(split(sums), axis=1), slide)

    firsts, seconds = boxes(first), boxes(second)
    totals = jnp.concatenate(
        [jnp.sum(chips.reshape(CHIP // 8, 8, band), axis=0),
         jnp.sum((chips * chips).reshape(CHIP // 8, 8, band), axis=0)], axis=0)
    totals = jnp.concatenate([totals[:, t * LANES:(t + 2) * LANES] for t in range(tiles)], axis=0)
    high, low = split(totals)
    rest = (totals - high.astype(F32) - low.astype(F32)).astype(BF16)
    totals = dot(jnp.concatenate([high, low, rest], axis=1), jnp.concatenate([table("gather")] * 3, axis=0))

    scores = []
    for t in range(tiles):
        first_t = firsts[t * LAGS:(t + 1) * LAGS]
        second_t = seconds[t * LAGS:(t + 1) * LAGS]
        total = jnp.sum(totals[16 * t:16 * t + 8], axis=0, keepdims=True)
        power = jnp.sum(totals[16 * t + 8:16 * t + 16], axis=0, keepdims=True)
        corr = raw[:, t * LANES:(t + 1) * LANES] - (total * (1.0 / AREA)) * first_t
        var_sum = second_t - first_t * first_t * (1.0 / AREA)
        energy = power - total * total * (1.0 / AREA)
        scores.append(CHIP * (corr * (1.0 / AREA)) * lax.rsqrt(
            (energy * (1.0 / AREA)) * (var_sum * (1.0 / AREA)) + EPSILON))
    high, low = split(jnp.concatenate(scores, axis=1))
    lifted = dot(table("cubic_rows"), jnp.concatenate([high, low], axis=0))
    cubic = jnp.concatenate([table("cubic_cols")] * 2, axis=0)
    half = (tiles + 1) // 2
    for begin, end in ((0, half), (half, tiles)):
        part = jnp.concatenate([lifted[:, t * LANES:(t + 1) * LANES] for t in range(begin, end)], axis=0)
        fine = dot(jnp.concatenate(split(part), axis=1), cubic)
        for t in range(begin, end):
            row = (t - begin) * CHIP
            out[0, 2 * t] = fine[row:row + CHIP, :CHIP]
            out[0, 2 * t + 1] = fine[row:row + CHIP, CHIP:]


def neighbours(axis):
    size = lax.axis_size(axis)
    forth = [(i, i + 1) for i in range(size - 1)]
    return forth, [(j, i) for i, j in forth]


def body(ref_image, sec_image, off_az, off_rg):
    rows, cols = ref_image.shape
    side = CHIP // 4
    chip_rows, chip_cols = rows // SPACE, cols // SPACE
    all_rows = chip_rows * lax.axis_size("az")
    reach = min(SPACE - 1, (all_rows - 1) // 2)
    pad = -(-(SPACE + reach) // 8) * 8
    assert SPACE + reach + side <= LANES
    tiles = cols // LANES

    tall = rows + 2 * pad

    def full(*shape):
        return jax.ShapeDtypeStruct(shape, F32)

    away = pl.BlockSpec(memory_space=pltpu.MemorySpace.HBM)
    sec, ref, to_up, to_down, to_right, to_left = pl.pallas_call(
        functools.partial(pack_kernel, pad, side),
        in_specs=[away] * 2,
        out_shape=[full(rows, cols)] * 2 + [full(pad + side, cols)] * 2 + [full(rows, LANES)] * 2,
        scratch_shapes=[pltpu.SemaphoreType.DMA((6,))],
        compiler_params=pltpu.CompilerParams(vmem_limit_bytes=8 << 20),
    )(*(pltpu.with_memory_space_constraint(x, pltpu.MemorySpace.HBM) for x in (sec_image, ref_image)))
    forth, back = neighbours("az")
    east, west = neighbours("rg")
    up = lax.ppermute(to_up, "az", forth)
    down = lax.ppermute(to_down, "az", back)
    left = lax.ppermute(to_right, "rg", east)
    right = lax.ppermute(to_left, "rg", west)
    corners_up, corners_down = pl.pallas_call(
        functools.partial(corner_kernel, pad),
        out_shape=[full(pad, 2 * LANES)] * 2,
        compiler_params=pltpu.CompilerParams(vmem_limit_bytes=8 << 20),
    )(left, right)
    corner_up = lax.ppermute(corners_up, "az", forth)
    corner_down = lax.ppermute(corners_down, "az", back)

    slab = jnp.asarray(tables()[0])
    held = pl.pallas_call(
        fetch_kernel,
        in_specs=[away],
        out_shape=jax.ShapeDtypeStruct(slab.shape, BF16),
        scratch_shapes=[pltpu.SemaphoreType.DMA],
        compiler_params=pltpu.CompilerParams(vmem_limit_bytes=8 << 20),
    )(pltpu.with_memory_space_constraint(slab, pltpu.MemorySpace.HBM))
    operands = [held, sec, ref, up, down, left, right, corner_up, corner_down]
    count = tiles + 1

    def whole(x):
        return pl.BlockSpec(x.shape, lambda i: (0, 0), pipeline_mode=pl.Buffered(1))

    return pl.pallas_call(
        functools.partial(main_kernel, pad, side),
        grid=(chip_rows,),
        in_specs=[away] * 2 + [whole(x) for x in operands],
        out_specs=pl.BlockSpec((1, chip_cols, 2 * LAGS, 2 * LAGS), lambda i: (i, 0, 0, 0)),
        scratch_shapes=[
            pltpu.SMEM((chip_rows,), jnp.int32),
            pltpu.SMEM((chip_rows,), jnp.int32),
            pltpu.VMEM((tall, cols + 2 * LANES), F32),
            pltpu.VMEM((rows + 2 * side, cols + LANES), F32),
            pltpu.VMEM((4 * count * FREQ, 2 * LANES), BF16),
            pltpu.VMEM((4 * count * FREQ, 2 * CHIP), F32),
            pltpu.VMEM((chip_cols * FREQ, 4 * CHIP), BF16),
            pltpu.SemaphoreType.DMA((3,)),
        ],
        out_shape=full(chip_rows, chip_cols, 2 * LAGS, 2 * LAGS),
        compiler_params=pltpu.CompilerParams(dimension_semantics=("arbitrary",), vmem_limit_bytes=40 << 20),
    )(*(pltpu.with_memory_space_constraint(x, pltpu.MemorySpace.HBM) for x in (off_az, off_rg)), *operands)


def solution(mesh):
    return jax.shard_map(
        body,
        mesh=mesh,
        in_specs=(P("az", "rg"), P("az", "rg"), P("az"), P("az")),
        out_specs=P("az", "rg", None, None),
        check_vma=False,
    )
```

```python
import functools
import math

import jax
import jax.numpy as jnp
import numpy as np
from jax import lax
from jax.experimental import pallas as pl
from jax.experimental.pallas import tpu as pltpu
from jax.sharding import PartitionSpec as P


CHIP = 128
SPACE = 64
SEARCH = 192
LAGS = 64
LANES = 128
FREQ = SEARCH // 2
EPSILON = 1e-06
AREA = float(CHIP * CHIP)
BF16 = jnp.bfloat16
F32 = jnp.float32


def halves(table):
    high = table.astype(BF16)
    low = (table - high.astype(np.float64)).astype(BF16)
    return high, low


@functools.cache
def tables():
    theta = 2.0 * math.pi * (np.arange(FREQ)[:, None] + 0.5) / SEARCH
    cell = np.arange(SEARCH)[None, :]
    forward = np.concatenate([np.cos(theta * cell), -np.sin(theta * cell)], axis=0)
    lag = np.arange(LAGS)[:, None]
    box = ((cell >= lag) & (cell < lag + CHIP)).astype(np.float64)
    made = {}
    high, low = halves(np.concatenate([forward, box], axis=0))
    made["rows_sec"] = np.concatenate([high, high, low], axis=1)
    high, low = halves(forward[:, :CHIP])
    made["rows_ref"] = np.concatenate([high, high, low], axis=1)
    made["rows_box"] = np.concatenate([box, box], axis=1).astype(BF16)

    phi = 2.0 * math.pi / CHIP * np.arange(CHIP)[None, :]
    spot = np.arange(SPACE)[:, None]
    cosine, sine = np.cos(phi * spot), np.sin(phi * spot)
    parts = (np.concatenate([cosine, -sine], axis=1), np.concatenate([sine, cosine], axis=1))
    made["columns"] = np.concatenate(halves(np.concatenate(parts, axis=0)), axis=0)

    cosine, sine = np.cos(phi.T * lag.T), np.sin(phi.T * lag.T)
    back = np.concatenate(
        [np.concatenate([cosine, sine], axis=1), np.concatenate([-sine, cosine], axis=1)], axis=0)
    made["back_columns"] = np.concatenate(halves(back), axis=1)

    final = np.concatenate([np.cos(theta.T * lag), -np.sin(theta.T * lag)], axis=1)
    high, low = halves(final * (2.0 / (SEARCH * CHIP)))
    made["back_rows"] = np.concatenate([high, high, low], axis=1)

    wide = np.arange(2 * LANES)[:, None]
    lane = np.arange(LANES)[None, :]
    start = lane // SPACE * SPACE
    made["slide"] = ((wide >= lane) & (wide < lane + CHIP)).astype(BF16)
    made["gather"] = ((wide >= start) & (wide < start + CHIP)).astype(BF16)

    out_index = np.arange(2 * LAGS)[:, None]
    sample = np.arange(LAGS)[None, :]
    base = out_index // 2

    def pick(where):
        return (np.clip(where, 0, LAGS - 1) == sample).astype(np.float64)

    odd = (9.0 * (pick(base) + pick(base + 1)) - (pick(base - 1) + pick(base + 2))) / 16.0
    cubic = np.where(out_index % 2 == 1, odd, pick(base))
    made["cubic_rows"] = np.concatenate([cubic, cubic], axis=1).astype(BF16)
    zero = np.zeros_like(cubic.T)
    made["cubic_cols"] = np.concatenate(
        [np.concatenate([cubic.T, zero], axis=1), np.concatenate([zero, cubic.T], axis=1)], axis=0
    ).astype(BF16)

    slabs, places, top = [], {}, 0
    for name, table in made.items():
        table = np.pad(table, ((0, 0), (0, -table.shape[1] % LANES)))
        pieces = [table[:, i:i + LANES] for i in range(0, table.shape[1], LANES)]
        places[name] = (top, table.shape[0], len(pieces), made[name].shape[1])
        slabs += pieces
        top += table.shape[0] * len(pieces)
    return np.concatenate(slabs, axis=0), places


def split(value):
    high = value.astype(BF16)
    low = (value - high.astype(F32)).astype(BF16)
    return high, low


def dot(left, right):
    return jnp.dot(left, right, preferred_element_type=F32)


def pack_kernel(pad, side, sec_hbm, ref_hbm, sec, ref, up, down, right, left, sems):
    rows, cols = sec.shape
    copies = [
        pltpu.make_async_copy(source, target, sems.at[i])
        for i, (source, target) in enumerate([
            (sec_hbm, sec),
            (ref_hbm, ref),
            (sec_hbm.at[pl.ds(rows - pad, pad)], up.at[pl.ds(0, pad)]),
            (sec_hbm.at[pl.ds(0, pad)], down.at[pl.ds(0, pad)]),
            (ref_hbm.at[pl.ds(rows - side, side)], up.at[pl.ds(pad, side)]),
            (ref_hbm.at[pl.ds(0, side)], down.at[pl.ds(pad, side)]),
        ])
    ]
    for copy in copies:
        copy.start()
    copies[0].wait()
    copies[1].wait()
    lane = lax.broadcasted_iota(jnp.int32, (1, LANES), 1)
    right[...] = jnp.where(lane >= side, sec[:, cols - LANES:], pltpu.roll(ref[:, cols - LANES:], side, 1))
    left[...] = jnp.where(lane < LANES - side, sec[:, :LANES], pltpu.roll(ref[:, :LANES], LANES - side, 1))
    for copy in copies[2:]:
        copy.wait()


def corner_kernel(pad, side, need, left, right, up, down):
    rows = left.shape[0]
    half = up.shape[0] - pad
    lane = lax.broadcasted_iota(jnp.int32, (1, LANES), 1)
    spare = LANES - need

    def tile(out, first, edge):
        west, east = left[first:first + pad], right[first:first + pad]
        out[0:pad] = jnp.where(lane < spare, east, west)
        upper = pltpu.roll(east[:half], (side - spare) % LANES, 1)
        lower = pltpu.roll(east[pad - half:], (2 * side - spare) % LANES, 1)
        inner = jnp.where(lane < 2 * side, upper, lower)
        inner = jnp.where(lane < side, west[edge:edge + half], inner)
        out[pad:] = jnp.where(lane < 3 * side, inner, east[edge:edge + half])

    tile(up, rows - pad, pad - half)
    tile(down, 0, 0)


def fetch_kernel(source, target, sem):
    copy = pltpu.make_async_copy(source, target, sem)
    copy.start()
    copy.wait()


def main_kernel(pad, side, need, off_az_hbm, off_rg_hbm, slab, sec, ref, up, down, left, right, corner_up,
                corner_down, out, off_az, off_rg, sec_ext, ref_ext, lhs, spec, zed, sems):
    rows, cols = sec.shape
    tiles = cols // LANES
    step = pl.program_id(0)
    band = cols + LANES

    def table(name):
        top, height, count, last = tables()[1][name]
        pieces = [slab[top + i * height:top + (i + 1) * height, :] for i in range(count)]
        value = jnp.concatenate(pieces, axis=1) if count > 1 else pieces[0]
        return value[:, :last]

    @pl.when(step == 0)
    def _():
        copies = [
            pltpu.make_async_copy(source, target, sems.at[i])
            for i, (source, target) in enumerate(
                [(off_az_hbm, off_az), (off_rg_hbm, off_rg)])
        ]
        for copy in copies:
            copy.start()
        level_sec = jnp.sum(sec[...]) * (1.0 / (rows * cols))
        level_ref = jnp.sum(ref[...]) * (1.0 / (rows * cols))
        inner = slice(LANES, LANES + cols)
        lane = lax.broadcasted_iota(jnp.int32, (1, LANES), 1)
        spare = LANES - need
        half = corner_up.shape[0] - pad

        def east_of(corner):
            rest = corner[pad:]
            upper = pltpu.roll(rest[:pad - half], (spare - side) % LANES, 1)
            lower = pltpu.roll(rest, (spare - 2 * side) % LANES, 1)
            return jnp.where(lane < spare, corner[0:pad], jnp.concatenate([upper, lower], axis=0))

        sec_ext[0:pad, 0:LANES] = corner_up[0:pad] - level_sec
        sec_ext[0:pad, inner] = up[0:pad] - level_sec
        sec_ext[0:pad, LANES + cols:] = east_of(corner_up) - level_sec
        sec_ext[pad:pad + rows, 0:LANES] = left[...] - level_sec
        sec_ext[pad:pad + rows, inner] = sec[...] - level_sec
        sec_ext[pad:pad + rows, LANES + cols:] = right[...] - level_sec
        sec_ext[pad + rows:, 0:LANES] = corner_down[0:pad] - level_sec
        sec_ext[pad + rows:, inner] = down[0:pad] - level_sec
        sec_ext[pad + rows:, LANES + cols:] = east_of(corner_down) - level_sec

        def place(at, west, middle, east):
            pieces = [pltpu.roll(west, LANES - side, 1)]
            pieces += [middle[:, t * LANES:(t + 1) * LANES] for t in range(tiles)]
            pieces += [pltpu.roll(east, side, 1)]
            turned = [pltpu.roll(piece, side, 1) for piece in pieces]
            for t in range(tiles + 1):
                ref_ext[at:at + west.shape[0], t * LANES:(t + 1) * LANES] = jnp.where(
                    lane < side, turned[t], turned[t + 1]) - level_ref

        place(0, corner_up[pad + half - side:], up[pad:], corner_up[pad + half - side:])
        place(side, left[...], ref[...], right[...])
        place(side + rows, corner_down[pad:pad + side], down[pad:], corner_down[pad:pad + side])
        for copy in copies:
            copy.wait()

    count = tiles + 1

    lane = lax.broadcasted_iota(jnp.int32, (1, LANES), 1)
    both = table("columns")
    major, minor = jnp.concatenate([both[:LANES]] * 2, axis=0), both[LANES:]

    def spread(which, source):
        for t in range(count):
            here = slice(t * LANES, (t + 1) * LANES)
            real, imag = source[:FREQ, here], source[FREQ:2 * FREQ, here]
            even = jnp.where(lane < SPACE, real, pltpu.roll(imag, SPACE, 1))
            odd = jnp.where(lane < SPACE, pltpu.roll(real, SPACE, 1), imag)
            for i, value in enumerate((even, odd)):
                row = ((which * count + t) * 2 + i) * FREQ
                lhs[row:row + FREQ, :] = jnp.concatenate(split(value), axis=1)
        for i in range(2):
            low = (which * 2 + i) * count * FREQ
            here = slice(low, low + count * FREQ)
            spec[here, :] = dot(lhs[here, :], major) + dot(lhs[here, :LANES], minor)

    chips = ref_ext[pl.ds(pl.multiple_of(step * SPACE, SPACE), CHIP), :]
    high, low = split(chips)
    spread(1, dot(table("rows_ref"), jnp.concatenate([high, low, high], axis=0)))

    start = step * SPACE + (pad - SPACE) + off_az[step]
    aligned = pl.multiple_of(start // 8 * 8, 8)
    field = sec_ext[pl.ds(aligned, SEARCH + 8), :]
    shift = LANES - SPACE - off_rg[step]
    turned = [pltpu.roll(field[:, t * LANES:(t + 1) * LANES], shift, 1) for t in range(tiles + 2)]
    lane = lax.broadcasted_iota(jnp.int32, (1, LANES), 1)
    field = jnp.concatenate(
        [jnp.where(lane < shift, turned[t], turned[t + 1]) for t in range(tiles + 1)], axis=1)
    part = start - aligned
    field = pltpu.roll(field.reshape(SEARCH // 8 + 1, 8, band), 8 - part, 1)
    line = lax.broadcasted_iota(jnp.int32, (1, 8, 1), 1)
    field = jnp.where(line < 8 - part, field[:-1], field[1:]).reshape(SEARCH, band)
    high, low = split(field)
    spectrum = dot(table("rows_sec"), jnp.concatenate([high, low, high], axis=0))
    square_high, square_low = split(field * field)
    second = dot(table("rows_box"), jnp.concatenate([square_high, square_low], axis=0))
    first = spectrum[2 * FREQ:]
    spread(0, spectrum)

    sign = (1 - 2 * (lax.broadcasted_iota(jnp.int32, (1, LANES), 1) % 2)).astype(F32)

    def block(which, b):
        row = (which * count * 2 + b) * FREQ
        return spec[row:row + FREQ, :CHIP], spec[row:row + FREQ, CHIP:]

    def product(b):
        (w_re, w_im), (n_re, n_im), (c_re, c_im) = block(0, b), block(0, b + 1), block(1, b)
        p_re, p_im = w_re + sign * n_re, w_im + sign * n_im
        return c_re * p_re + c_im * p_im, c_re * p_im - c_im * p_re

    chips_here = 2 * tiles
    before = product(0)
    for c in range(chips_here):
        after = product(c + 1)
        both = jnp.concatenate([before[0] + after[0], before[1] + after[1]], axis=1)
        high, low = split(both)
        row = c * FREQ
        zed[row:row + FREQ, :2 * CHIP] = high
        zed[row:row + FREQ, 2 * CHIP:] = low
        before = after
    back = table("back_columns")
    main = dot(zed[:, :2 * CHIP], back)
    rest = dot(zed[:, 2 * CHIP:], back[:, :2 * LAGS])
    pieces = []
    for t in range(tiles):
        pair = []
        for row in (2 * t * FREQ, (2 * t + 1) * FREQ):
            here = main[row:row + FREQ]
            pair.append(here[:, :LANES] + here[:, LANES:] + rest[row:row + FREQ])
        even, odd = pair[0], pair[1]
        odd_turned, even_turned = pltpu.roll(odd, LAGS, 1), pltpu.roll(even, LAGS, 1)
        pieces.append(jnp.concatenate(
            [jnp.where(lane < LAGS, even, odd_turned), jnp.where(lane < LAGS, even_turned, odd)], axis=0))
    stacked = jnp.concatenate(pieces, axis=1)
    high, low = split(stacked)
    raw = dot(table("back_rows"), jnp.concatenate([high, low, high], axis=0))

    slide = jnp.concatenate([table("slide")] * 2, axis=0)

    def boxes(sums):
        sums = jnp.concatenate([sums[:, t * LANES:(t + 2) * LANES] for t in range(tiles)], axis=0)
        return dot(jnp.concatenate(split(sums), axis=1), slide)

    firsts, seconds = boxes(first), boxes(second)
    totals = jnp.concatenate(
        [jnp.sum(chips.reshape(CHIP // 8, 8, band), axis=0),
         jnp.sum((chips * chips).reshape(CHIP // 8, 8, band), axis=0)], axis=0)
    totals = jnp.concatenate([totals[:, t * LANES:(t + 2) * LANES] for t in range(tiles)], axis=0)
    high, low = split(totals)
    rest = (totals - high.astype(F32) - low.astype(F32)).astype(BF16)
    totals = dot(jnp.concatenate([high, low, rest], axis=1), jnp.concatenate([table("gather")] * 3, axis=0))

    scores = []
    for t in range(tiles):
        first_t = firsts[t * LAGS:(t + 1) * LAGS]
        second_t = seconds[t * LAGS:(t + 1) * LAGS]
        total = jnp.sum(totals[16 * t:16 * t + 8], axis=0, keepdims=True)
        power = jnp.sum(totals[16 * t + 8:16 * t + 16], axis=0, keepdims=True)
        corr = raw[:, t * LANES:(t + 1) * LANES] - (total * (1.0 / AREA)) * first_t
        var_sum = second_t - first_t * first_t * (1.0 / AREA)
        energy = power - total * total * (1.0 / AREA)
        scores.append(CHIP * (corr * (1.0 / AREA)) * lax.rsqrt(
            (energy * (1.0 / AREA)) * (var_sum * (1.0 / AREA)) + EPSILON))
    high, low = split(jnp.concatenate(scores, axis=1))
    lifted = dot(table("cubic_rows"), jnp.concatenate([high, low], axis=0))
    cubic = jnp.concatenate([table("cubic_cols")] * 2, axis=0)
    half = (tiles + 1) // 2
    for begin, end in ((0, half), (half, tiles)):
        part = jnp.concatenate([lifted[:, t * LANES:(t + 1) * LANES] for t in range(begin, end)], axis=0)
        fine = dot(jnp.concatenate(split(part), axis=1), cubic)
        for t in range(begin, end):
            row = (t - begin) * CHIP
            out[0, 2 * t] = fine[row:row + CHIP, :CHIP]
            out[0, 2 * t + 1] = fine[row:row + CHIP, CHIP:]


def neighbours(axis):
    size = lax.axis_size(axis)
    forth = [(i, i + 1) for i in range(size - 1)]
    return forth, [(j, i) for i, j in forth]


def body(ref_image, sec_image, off_az, off_rg):
    rows, cols = ref_image.shape
    side = CHIP // 4
    chip_rows, chip_cols = rows // SPACE, cols // SPACE
    all_rows = chip_rows * lax.axis_size("az")
    reach = min(SPACE - 1, (all_rows - 1) // 2)
    pad = -(-(SPACE + reach) // 8) * 8
    need = SPACE + reach
    half = -(-pad // 16) * 8
    assert need + side <= LANES and half >= side and 2 * need - LANES <= side
    tiles = cols // LANES

    tall = rows + 2 * pad

    def full(*shape):
        return jax.ShapeDtypeStruct(shape, F32)

    away = pl.BlockSpec(memory_space=pltpu.MemorySpace.HBM)
    sec, ref, to_up, to_down, to_right, to_left = pl.pallas_call(
        functools.partial(pack_kernel, pad, side),
        in_specs=[away] * 2,
        out_shape=[full(rows, cols)] * 2 + [full(pad + side, cols)] * 2 + [full(rows, LANES)] * 2,
        scratch_shapes=[pltpu.SemaphoreType.DMA((6,))],
        compiler_params=pltpu.CompilerParams(vmem_limit_bytes=8 << 20),
    )(*(pltpu.with_memory_space_constraint(x, pltpu.MemorySpace.HBM) for x in (sec_image, ref_image)))
    forth, back = neighbours("az")
    east, west = neighbours("rg")
    up = lax.ppermute(to_up, "az", forth)
    down = lax.ppermute(to_down, "az", back)
    left = lax.ppermute(to_right, "rg", east)
    right = lax.ppermute(to_left, "rg", west)
    corners_up, corners_down = pl.pallas_call(
        functools.partial(corner_kernel, pad, side, need),
        out_shape=[full(pad + half, LANES)] * 2,
        compiler_params=pltpu.CompilerParams(vmem_limit_bytes=8 << 20),
    )(left, right)
    corner_up = lax.ppermute(corners_up, "az", forth)
    corner_down = lax.ppermute(corners_down, "az", back)

    slab = jnp.asarray(tables()[0])
    held = pl.pallas_call(
        fetch_kernel,
        in_specs=[away],
        out_shape=jax.ShapeDtypeStruct(slab.shape, BF16),
        scratch_shapes=[pltpu.SemaphoreType.DMA],
        compiler_params=pltpu.CompilerParams(vmem_limit_bytes=8 << 20),
    )(pltpu.with_memory_space_constraint(slab, pltpu.MemorySpace.HBM))
    operands = [held, sec, ref, up, down, left, right, corner_up, corner_down]
    count = tiles + 1

    def whole(x):
        return pl.BlockSpec(x.shape, lambda i: (0, 0), pipeline_mode=pl.Buffered(1))

    return pl.pallas_call(
        functools.partial(main_kernel, pad, side, need),
        grid=(chip_rows,),
        in_specs=[away] * 2 + [whole(x) for x in operands],
        out_specs=pl.BlockSpec((1, chip_cols, 2 * LAGS, 2 * LAGS), lambda i: (i, 0, 0, 0)),
        scratch_shapes=[
            pltpu.SMEM((chip_rows,), jnp.int32),
            pltpu.SMEM((chip_rows,), jnp.int32),
            pltpu.VMEM((tall, cols + 2 * LANES), F32),
            pltpu.VMEM((rows + 2 * side, cols + LANES), F32),
            pltpu.VMEM((4 * count * FREQ, 2 * LANES), BF16),
            pltpu.VMEM((4 * count * FREQ, 2 * CHIP), F32),
            pltpu.VMEM((chip_cols * FREQ, 4 * CHIP), BF16),
            pltpu.SemaphoreType.DMA((3,)),
        ],
        out_shape=full(chip_rows, chip_cols, 2 * LAGS, 2 * LAGS),
        compiler_params=pltpu.CompilerParams(dimension_semantics=("arbitrary",), vmem_limit_bytes=40 << 20),
    )(*(pltpu.with_memory_space_constraint(x, pltpu.MemorySpace.HBM) for x in (off_az, off_rg)), *operands)


def solution(mesh):
    return jax.shard_map(
        body,
        mesh=mesh,
        in_specs=(P("az", "rg"), P("az", "rg"), P("az"), P("az")),
        out_specs=P("az", "rg", None, None),
        check_vma=False,
    )
```

```python
import functools
import math

import jax
import jax.numpy as jnp
import numpy as np
from jax import lax
from jax.experimental import pallas as pl
from jax.experimental.pallas import tpu as pltpu
from jax.sharding import PartitionSpec as P


CHIP = 128
SPACE = 64
SEARCH = 192
LAGS = 64
LANES = 128
FREQ = SEARCH // 2
EPSILON = 1e-06
AREA = float(CHIP * CHIP)
BF16 = jnp.bfloat16
F32 = jnp.float32


def halves(table):
    high = table.astype(BF16)
    low = (table - high.astype(np.float64)).astype(BF16)
    return high, low


@functools.cache
def tables():
    theta = 2.0 * math.pi * (np.arange(FREQ)[:, None] + 0.5) / SEARCH
    cell = np.arange(SEARCH)[None, :]
    forward = np.concatenate([np.cos(theta * cell), -np.sin(theta * cell)], axis=0)
    lag = np.arange(LAGS)[:, None]
    box = ((cell >= lag) & (cell < lag + CHIP)).astype(np.float64)
    made = {}
    high, low = halves(np.concatenate([forward, box], axis=0))
    made["rows_sec"] = np.concatenate([high, high, low], axis=1)
    high, low = halves(forward[:, :CHIP])
    made["rows_ref"] = np.concatenate([high, high, low], axis=1)
    made["rows_box"] = np.concatenate([box, box], axis=1).astype(BF16)

    phi = 2.0 * math.pi / CHIP * np.arange(CHIP)[None, :]
    spot = np.arange(SPACE)[:, None]
    cosine, sine = np.cos(phi * spot), np.sin(phi * spot)
    parts = (np.concatenate([cosine, -sine], axis=1), np.concatenate([sine, cosine], axis=1))
    made["columns"] = np.concatenate(halves(np.concatenate(parts, axis=0)), axis=0)

    cosine, sine = np.cos(phi.T * lag.T), np.sin(phi.T * lag.T)
    back = np.concatenate(
        [np.concatenate([cosine, sine], axis=1), np.concatenate([-sine, cosine], axis=1)], axis=0)
    made["back_columns"] = np.concatenate(halves(back), axis=1)

    final = np.concatenate([np.cos(theta.T * lag), -np.sin(theta.T * lag)], axis=1)
    high, low = halves(final * (2.0 / (SEARCH * CHIP)))
    made["back_rows"] = np.concatenate([high, high, low], axis=1)

    wide = np.arange(2 * LANES)[:, None]
    lane = np.arange(LANES)[None, :]
    start = lane // SPACE * SPACE
    made["slide"] = ((wide >= lane) & (wide < lane + CHIP)).astype(BF16)
    made["gather"] = ((wide >= start) & (wide < start + CHIP)).astype(BF16)

    out_index = np.arange(2 * LAGS)[:, None]
    sample = np.arange(LAGS)[None, :]
    base = out_index // 2

    def pick(where):
        return (np.clip(where, 0, LAGS - 1) == sample).astype(np.float64)

    odd = (9.0 * (pick(base) + pick(base + 1)) - (pick(base - 1) + pick(base + 2))) / 16.0
    cubic = np.where(out_index % 2 == 1, odd, pick(base))
    made["cubic_rows"] = np.concatenate([cubic, cubic], axis=1).astype(BF16)
    zero = np.zeros_like(cubic.T)
    made["cubic_cols"] = np.concatenate(
        [np.concatenate([cubic.T, zero], axis=1), np.concatenate([zero, cubic.T], axis=1)], axis=0
    ).astype(BF16)

    slabs, places, top = [], {}, 0
    for name, table in made.items():
        table = np.pad(table, ((0, 0), (0, -table.shape[1] % LANES)))
        pieces = [table[:, i:i + LANES] for i in range(0, table.shape[1], LANES)]
        places[name] = (top, table.shape[0], len(pieces), made[name].shape[1])
        slabs += pieces
        top += table.shape[0] * len(pieces)
    return np.concatenate(slabs, axis=0), places


def split(value):
    high = value.astype(BF16)
    low = (value - high.astype(F32)).astype(BF16)
    return high, low


def dot(left, right):
    return jnp.dot(left, right, preferred_element_type=F32)


def pack_kernel(pad, side, sec_hbm, ref_hbm, sec, ref, up, down, right, left, sems):
    rows, cols = sec.shape
    copies = [
        pltpu.make_async_copy(source, target, sems.at[i])
        for i, (source, target) in enumerate([
            (sec_hbm, sec),
            (ref_hbm, ref),
            (sec_hbm.at[pl.ds(rows - pad, pad)], up.at[pl.ds(0, pad)]),
            (sec_hbm.at[pl.ds(0, pad)], down.at[pl.ds(0, pad)]),
            (ref_hbm.at[pl.ds(rows - side, side)], up.at[pl.ds(pad, side)]),
            (ref_hbm.at[pl.ds(0, side)], down.at[pl.ds(pad, side)]),
        ])
    ]
    for copy in copies:
        copy.start()
    copies[0].wait()
    copies[1].wait()
    lane = lax.broadcasted_iota(jnp.int32, (1, LANES), 1)
    right[...] = jnp.where(lane >= side, sec[:, cols - LANES:], pltpu.roll(ref[:, cols - LANES:], side, 1))
    left[...] = jnp.where(lane < LANES - side, sec[:, :LANES], pltpu.roll(ref[:, :LANES], LANES - side, 1))
    for copy in copies[2:]:
        copy.wait()


def corner_kernel(pad, side, need, left, right, up, down):
    rows = left.shape[0]
    half = up.shape[0] - pad
    lane = lax.broadcasted_iota(jnp.int32, (1, LANES), 1)
    spare = LANES - need

    def tile(out, first, edge):
        west, east = left[first:first + pad], right[first:first + pad]
        out[0:pad] = jnp.where(lane < spare, east, west)
        upper = pltpu.roll(east[:half], (side - spare) % LANES, 1)
        lower = pltpu.roll(east[pad - half:], (2 * side - spare) % LANES, 1)
        inner = jnp.where(lane < 2 * side, upper, lower)
        inner = jnp.where(lane < side, west[edge:edge + half], inner)
        out[pad:] = jnp.where(lane < 3 * side, inner, east[edge:edge + half])

    tile(up, rows - pad, pad - half)
    tile(down, 0, 0)


def fetch_kernel(source, sec, ref, target, levels, sem):
    copy = pltpu.make_async_copy(source, target, sem)
    copy.start()
    scale = 1.0 / (sec.shape[0] * sec.shape[1])
    levels[0:8] = jnp.full((8, LANES), jnp.sum(sec[...]) * scale, F32)
    levels[8:16] = jnp.full((8, LANES), jnp.sum(ref[...]) * scale, F32)
    copy.wait()


def main_kernel(pad, side, need, off_az_hbm, off_rg_hbm, slab, levels, sec, ref, up, down, left, right, corner_up,
                corner_down, out, off_az, off_rg, sec_ext, ref_ext, lhs, spec, zed, sems):
    rows, cols = sec.shape
    tiles = cols // LANES
    step = pl.program_id(0)
    band = cols + LANES

    def table(name):
        top, height, count, last = tables()[1][name]
        pieces = [slab[top + i * height:top + (i + 1) * height, :] for i in range(count)]
        value = jnp.concatenate(pieces, axis=1) if count > 1 else pieces[0]
        return value[:, :last]

    @pl.when(step == 0)
    def _():
        copies = [
            pltpu.make_async_copy(source, target, sems.at[i])
            for i, (source, target) in enumerate(
                [(off_az_hbm, off_az), (off_rg_hbm, off_rg)])
        ]
        for copy in copies:
            copy.start()
        level_sec, level_ref = levels[0:1], levels[8:9]
        level_wide = jnp.concatenate([level_sec] * tiles, axis=1)
        inner = slice(LANES, LANES + cols)
        lane = lax.broadcasted_iota(jnp.int32, (1, LANES), 1)
        spare = LANES - need
        half = corner_up.shape[0] - pad

        def east_of(corner):
            rest = corner[pad:]
            upper = pltpu.roll(rest[:pad - half], (spare - side) % LANES, 1)
            lower = pltpu.roll(rest, (spare - 2 * side) % LANES, 1)
            return jnp.where(lane < spare, corner[0:pad], jnp.concatenate([upper, lower], axis=0))

        sec_ext[0:pad, 0:LANES] = corner_up[0:pad] - level_sec
        sec_ext[0:pad, inner] = up[0:pad] - level_wide
        sec_ext[0:pad, LANES + cols:] = east_of(corner_up) - level_sec
        sec_ext[pad:pad + rows, 0:LANES] = left[...] - level_sec
        sec_ext[pad:pad + rows, inner] = sec[...] - level_wide
        sec_ext[pad:pad + rows, LANES + cols:] = right[...] - level_sec
        sec_ext[pad + rows:, 0:LANES] = corner_down[0:pad] - level_sec
        sec_ext[pad + rows:, inner] = down[0:pad] - level_wide
        sec_ext[pad + rows:, LANES + cols:] = east_of(corner_down) - level_sec

        def place(at, west, middle, east):
            pieces = [pltpu.roll(west, LANES - side, 1)]
            pieces += [middle[:, t * LANES:(t + 1) * LANES] for t in range(tiles)]
            pieces += [pltpu.roll(east, side, 1)]
            turned = [pltpu.roll(piece, side, 1) for piece in pieces]
            for t in range(tiles + 1):
                ref_ext[at:at + west.shape[0], t * LANES:(t + 1) * LANES] = jnp.where(
                    lane < side, turned[t], turned[t + 1]) - level_ref

        place(0, corner_up[pad + half - side:], up[pad:], corner_up[pad + half - side:])
        place(side, left[...], ref[...], right[...])
        place(side + rows, corner_down[pad:pad + side], down[pad:], corner_down[pad:pad + side])
        for copy in copies:
            copy.wait()

    count = tiles + 1

    lane = lax.broadcasted_iota(jnp.int32, (1, LANES), 1)
    both = table("columns")
    major, minor = jnp.concatenate([both[:LANES]] * 2, axis=0), both[LANES:]

    def spread(which, source):
        for t in range(count):
            here = slice(t * LANES, (t + 1) * LANES)
            real, imag = source[:FREQ, here], source[FREQ:2 * FREQ, here]
            even = jnp.where(lane < SPACE, real, pltpu.roll(imag, SPACE, 1))
            odd = jnp.where(lane < SPACE, pltpu.roll(real, SPACE, 1), imag)
            for i, value in enumerate((even, odd)):
                row = ((which * count + t) * 2 + i) * FREQ
                lhs[row:row + FREQ, :] = jnp.concatenate(split(value), axis=1)
        for i in range(2):
            low = (which * 2 + i) * count * FREQ
            here = slice(low, low + count * FREQ)
            spec[here, :] = dot(lhs[here, :], major) + dot(lhs[here, :LANES], minor)

    chips = ref_ext[pl.ds(pl.multiple_of(step * SPACE, SPACE), CHIP), :]
    high, low = split(chips)
    spread(1, dot(table("rows_ref"), jnp.concatenate([high, low, high], axis=0)))

    start = step * SPACE + (pad - SPACE) + off_az[step]
    aligned = pl.multiple_of(start // 8 * 8, 8)
    field = sec_ext[pl.ds(aligned, SEARCH + 8), :]
    shift = LANES - SPACE - off_rg[step]
    turned = [pltpu.roll(field[:, t * LANES:(t + 1) * LANES], shift, 1) for t in range(tiles + 2)]
    lane = lax.broadcasted_iota(jnp.int32, (1, LANES), 1)
    field = jnp.concatenate(
        [jnp.where(lane < shift, turned[t], turned[t + 1]) for t in range(tiles + 1)], axis=1)
    part = start - aligned
    field = pltpu.roll(field.reshape(SEARCH // 8 + 1, 8, band), 8 - part, 1)
    line = lax.broadcasted_iota(jnp.int32, (1, 8, 1), 1)
    field = jnp.where(line < 8 - part, field[:-1], field[1:]).reshape(SEARCH, band)
    high, low = split(field)
    spectrum = dot(table("rows_sec"), jnp.concatenate([high, low, high], axis=0))
    square_high, square_low = split(field * field)
    second = dot(table("rows_box"), jnp.concatenate([square_high, square_low], axis=0))
    first = spectrum[2 * FREQ:]
    spread(0, spectrum)

    sign = (1 - 2 * (lax.broadcasted_iota(jnp.int32, (1, LANES), 1) % 2)).astype(F32)

    def block(which, b):
        row = (which * count * 2 + b) * FREQ
        return spec[row:row + FREQ, :CHIP], spec[row:row + FREQ, CHIP:]

    def product(b):
        (w_re, w_im), (n_re, n_im), (c_re, c_im) = block(0, b), block(0, b + 1), block(1, b)
        p_re, p_im = w_re + sign * n_re, w_im + sign * n_im
        return c_re * p_re + c_im * p_im, c_re * p_im - c_im * p_re

    chips_here = 2 * tiles
    before = product(0)
    for c in range(chips_here):
        after = product(c + 1)
        both = jnp.concatenate([before[0] + after[0], before[1] + after[1]], axis=1)
        high, low = split(both)
        row = c * FREQ
        zed[row:row + FREQ, :2 * CHIP] = high
        zed[row:row + FREQ, 2 * CHIP:] = low
        before = after
    back = table("back_columns")
    main = dot(zed[:, :2 * CHIP], back)
    rest = dot(zed[:, 2 * CHIP:], back[:, :2 * LAGS])
    pieces = []
    for t in range(tiles):
        pair = []
        for row in (2 * t * FREQ, (2 * t + 1) * FREQ):
            here = main[row:row + FREQ]
            pair.append(here[:, :LANES] + here[:, LANES:] + rest[row:row + FREQ])
        even, odd = pair[0], pair[1]
        odd_turned, even_turned = pltpu.roll(odd, LAGS, 1), pltpu.roll(even, LAGS, 1)
        pieces.append(jnp.concatenate(
            [jnp.where(lane < LAGS, even, odd_turned), jnp.where(lane < LAGS, even_turned, odd)], axis=0))
    stacked = jnp.concatenate(pieces, axis=1)
    high, low = split(stacked)
    raw = dot(table("back_rows"), jnp.concatenate([high, low, high], axis=0))

    slide = jnp.concatenate([table("slide")] * 2, axis=0)

    def boxes(sums):
        sums = jnp.concatenate([sums[:, t * LANES:(t + 2) * LANES] for t in range(tiles)], axis=0)
        return dot(jnp.concatenate(split(sums), axis=1), slide)

    firsts, seconds = boxes(first), boxes(second)
    totals = jnp.concatenate(
        [jnp.sum(chips.reshape(CHIP // 8, 8, band), axis=0),
         jnp.sum((chips * chips).reshape(CHIP // 8, 8, band), axis=0)], axis=0)
    totals = jnp.concatenate([totals[:, t * LANES:(t + 2) * LANES] for t in range(tiles)], axis=0)
    high, low = split(totals)
    rest = (totals - high.astype(F32) - low.astype(F32)).astype(BF16)
    totals = dot(jnp.concatenate([high, low, rest], axis=1), jnp.concatenate([table("gather")] * 3, axis=0))

    scores = []
    for t in range(tiles):
        first_t = firsts[t * LAGS:(t + 1) * LAGS]
        second_t = seconds[t * LAGS:(t + 1) * LAGS]
        total = jnp.sum(totals[16 * t:16 * t + 8], axis=0, keepdims=True)
        power = jnp.sum(totals[16 * t + 8:16 * t + 16], axis=0, keepdims=True)
        corr = raw[:, t * LANES:(t + 1) * LANES] - (total * (1.0 / AREA)) * first_t
        var_sum = second_t - first_t * first_t * (1.0 / AREA)
        energy = power - total * total * (1.0 / AREA)
        scores.append(CHIP * (corr * (1.0 / AREA)) * lax.rsqrt(
            (energy * (1.0 / AREA)) * (var_sum * (1.0 / AREA)) + EPSILON))
    high, low = split(jnp.concatenate(scores, axis=1))
    lifted = dot(table("cubic_rows"), jnp.concatenate([high, low], axis=0))
    cubic = jnp.concatenate([table("cubic_cols")] * 2, axis=0)
    half = (tiles + 1) // 2
    for begin, end in ((0, half), (half, tiles)):
        part = jnp.concatenate([lifted[:, t * LANES:(t + 1) * LANES] for t in range(begin, end)], axis=0)
        fine = dot(jnp.concatenate(split(part), axis=1), cubic)
        for t in range(begin, end):
            row = (t - begin) * CHIP
            out[0, 2 * t] = fine[row:row + CHIP, :CHIP]
            out[0, 2 * t + 1] = fine[row:row + CHIP, CHIP:]


def neighbours(axis):
    size = lax.axis_size(axis)
    forth = [(i, i + 1) for i in range(size - 1)]
    return forth, [(j, i) for i, j in forth]


def body(ref_image, sec_image, off_az, off_rg):
    rows, cols = ref_image.shape
    side = CHIP // 4
    chip_rows, chip_cols = rows // SPACE, cols // SPACE
    all_rows = chip_rows * lax.axis_size("az")
    reach = min(SPACE - 1, (all_rows - 1) // 2)
    pad = -(-(SPACE + reach) // 8) * 8
    need = SPACE + reach
    half = -(-pad // 16) * 8
    assert need + side <= LANES and half >= side and 2 * need - LANES <= side
    tiles = cols // LANES

    tall = rows + 2 * pad

    def full(*shape):
        return jax.ShapeDtypeStruct(shape, F32)

    away = pl.BlockSpec(memory_space=pltpu.MemorySpace.HBM)
    sec, ref, to_up, to_down, to_right, to_left = pl.pallas_call(
        functools.partial(pack_kernel, pad, side),
        in_specs=[away] * 2,
        out_shape=[full(rows, cols)] * 2 + [full(pad + side, cols)] * 2 + [full(rows, LANES)] * 2,
        scratch_shapes=[pltpu.SemaphoreType.DMA((6,))],
        compiler_params=pltpu.CompilerParams(vmem_limit_bytes=8 << 20),
    )(*(pltpu.with_memory_space_constraint(x, pltpu.MemorySpace.HBM) for x in (sec_image, ref_image)))
    forth, back = neighbours("az")
    east, west = neighbours("rg")
    up = lax.ppermute(to_up, "az", forth)
    down = lax.ppermute(to_down, "az", back)
    left = lax.ppermute(to_right, "rg", east)
    right = lax.ppermute(to_left, "rg", west)
    corners_up, corners_down = pl.pallas_call(
        functools.partial(corner_kernel, pad, side, need),
        out_shape=[full(pad + half, LANES)] * 2,
        compiler_params=pltpu.CompilerParams(vmem_limit_bytes=8 << 20),
    )(left, right)
    corner_up = lax.ppermute(corners_up, "az", forth)
    corner_down = lax.ppermute(corners_down, "az", back)

    slab = jnp.asarray(tables()[0])
    held, levels = pl.pallas_call(
        fetch_kernel,
        in_specs=[away] + [pl.BlockSpec(memory_space=pltpu.MemorySpace.VMEM)] * 2,
        out_shape=[jax.ShapeDtypeStruct(slab.shape, BF16), full(16, LANES)],
        scratch_shapes=[pltpu.SemaphoreType.DMA],
        compiler_params=pltpu.CompilerParams(vmem_limit_bytes=8 << 20),
    )(pltpu.with_memory_space_constraint(slab, pltpu.MemorySpace.HBM), sec, ref)
    operands = [held, levels, sec, ref, up, down, left, right, corner_up, corner_down]
    count = tiles + 1

    def whole(x):
        return pl.BlockSpec(x.shape, lambda i: (0, 0), pipeline_mode=pl.Buffered(1))

    return pl.pallas_call(
        functools.partial(main_kernel, pad, side, need),
        grid=(chip_rows,),
        in_specs=[away] * 2 + [whole(x) for x in operands],
        out_specs=pl.BlockSpec((1, chip_cols, 2 * LAGS, 2 * LAGS), lambda i: (i, 0, 0, 0)),
        scratch_shapes=[
            pltpu.SMEM((chip_rows,), jnp.int32),
            pltpu.SMEM((chip_rows,), jnp.int32),
            pltpu.VMEM((tall, cols + 2 * LANES), F32),
            pltpu.VMEM((rows + 2 * side, cols + LANES), F32),
            pltpu.VMEM((4 * count * FREQ, 2 * LANES), BF16),
            pltpu.VMEM((4 * count * FREQ, 2 * CHIP), F32),
            pltpu.VMEM((chip_cols * FREQ, 4 * CHIP), BF16),
            pltpu.SemaphoreType.DMA((3,)),
        ],
        out_shape=full(chip_rows, chip_cols, 2 * LAGS, 2 * LAGS),
        compiler_params=pltpu.CompilerParams(dimension_semantics=("arbitrary",), vmem_limit_bytes=40 << 20),
    )(*(pltpu.with_memory_space_constraint(x, pltpu.MemorySpace.HBM) for x in (off_az, off_rg)), *operands)


def solution(mesh):
    return jax.shard_map(
        body,
        mesh=mesh,
        in_specs=(P("az", "rg"), P("az", "rg"), P("az"), P("az")),
        out_specs=P("az", "rg", None, None),
        check_vma=False,
    )
```
